512 devices in a mesh: row: 8 (over x, core), col: 16 (over z), gz: 4 (over y).
Axes of the slice: x: 4, y: 4, z: 16, core: 2. Of those that a mesh axis runs over, the one named last changes fastest.
Arguments:
- density_matrix: bfloat16 [8192, 8192], P('row', 'col'), may hold values from -24 to 24
- block_pattern: int32 [128, 128], P('row', 'col'), may hold values from 0 to 1, as said below
- tile_lists: int32 [512, 16], replicated, may hold values from 0 to 127, as said below
- basis_values: bfloat16 [8, 16, 4, 1024, 384], P('row', 'col', 'gz'), may hold values from -0.09375 to 0.09375
- core_density: float32 [16, 128, 96], P('row', 'col', 'gz'), may hold values from 0.5 to 4
- orbitals: float32 [8192, 128], P(('col', 'gz')), may hold values from -6 to 6
Outputs:
- hamiltonian: float32 [8192, 8192], P('row', ('col', 'gz'))
- applied: float32 [8192, 128], P(('row', 'col', 'gz'))
The draws below stay inside these ranges and needn't reach their ends.
Inputs may be any that keep to these rules, and one draw needn't show every extreme that they name: `block_pattern`: Symmetric, with ones on the diagonal. `tile_lists`: each row is increasing and holds exactly 1 block ids from every run of 8 ids that starts at a multiple of 8.
All inputs are finite; a program needn't handle non-finite values.
Results may differ from the reference program's by a relative error of at most 0.00048.
Values may be sent and summed in bfloat16 or wider, within the bound.
No kernel may reach another device: no remote copies, remote signals or barrier semaphores. Data moves between devices by JAX's collectives and lax.ppermute only.
A program may use at most 64 MiB of HBM per device.

```python
import math
import jax
import jax.numpy as jnp
from jax import lax

NB = 8192
BS = 64
NORB = 128
TL = 16
TX = 2
TY = 8
TZ = 24
NBLK = 128
GROUP = 8
KC = 1
OV = 1024
CELLS = 384
NX = 16
NY = 128
NZ = 96
N_ROW = 8
N_COL = 16
N_GZ = 4
DEVICES = 512


def listed_blocks(key):
    key_list = jax.random.split(jax.random.fold_in(key, 17), DEVICES * N_COL)

    def choose(subkey):
        return jnp.sort(jax.random.permutation(subkey, GROUP)[:KC])
    chosen = jax.vmap(choose)(key_list).reshape(DEVICES, N_COL, KC).astype(jnp.int32)
    offsets = (jnp.arange(N_COL, dtype=jnp.int32) * GROUP)[None, :, None]
    return (chosen + offsets).reshape(DEVICES, TL).astype(jnp.int32)


def draw_tile_lists(key, part):
    return listed_blocks(key)


def draw_block_pattern(key, part):
    random_bits = jax.random.randint(jax.random.fold_in(key, 23), (NBLK, NBLK), 0, 2)
    row_ids = jnp.arange(NBLK, dtype=jnp.int32)[:, None]
    col_ids = jnp.arange(NBLK, dtype=jnp.int32)[None, :]
    mirrored = jnp.where(row_ids < col_ids, random_bits, random_bits.T)
    lists = listed_blocks(key)
    full_count = max(2, DEVICES // 64)
    full_tiles = jax.random.permutation(jax.random.fold_in(key, 29), DEVICES)[:full_count]
    full_lists = jnp.take(lists, full_tiles, axis=0)
    block_ids = jnp.arange(NBLK, dtype=jnp.int32)
    member = jnp.max((full_lists[:, :, None] == block_ids[None, None, :]).astype(jnp.int32), axis=1)
    covered = jnp.max(member[:, :, None] * member[:, None, :], axis=0)
    joined = jnp.maximum(mirrored, covered)
    return jnp.where(row_ids == col_ids, 1, joined).astype(jnp.int32)


def levels(rng, shape, cuts, low, largest):
    factor_of = 1.0
    for dim, shards_of in cuts:
        heights = jax.random.uniform(jax.random.fold_in(jax.random.fold_in(rng, 6), dim), (shards_of,), jnp.float32, low / len(cuts), largest / len(cuts))
        factor_of = factor_of * jnp.repeat(jnp.exp(heights), shape[dim] // shards_of).reshape((-1,) + (1,) * (len(shape) - 1 - dim))
    return factor_of


def scatter_about(own_key, dims, width, reach, cuts=(), held_as=jnp.bfloat16):
    factor_of = levels(own_key, dims, cuts, -0.22, 0.18) if cuts else 1.0
    array = jax.random.normal(own_key, dims, jnp.float32) * width * factor_of
    return jnp.minimum(jnp.maximum(array, -reach), reach).astype(held_as)


def setup_inputs(seed: int = 0) -> dict:
    seeds = jax.random.split(jax.random.key(seed), 7)
    density_matrix = scatter_about(seeds[0], (NB, NB), 4.0, 24.0, ((0, 8), (1, 16)))
    block_pattern = draw_block_pattern(jax.random.fold_in(seeds[6], 71), 0)
    tile_lists = draw_tile_lists(jax.random.fold_in(seeds[6], 71), 0)
    basis_values = scatter_about(seeds[3], (N_ROW, N_COL, N_GZ, OV, CELLS), 0.015625, 0.09375, ((0, 8), (1, 16), (2, 4)))
    core_density = jnp.clip(jnp.exp(math.log(4.0) - 2.0794415 * jax.random.uniform(seeds[4], (NX, NY, NZ), jnp.float32) ** levels(seeds[4], (NX, NY, NZ), ((0, 8), (1, 16), (2, 4)), -0.2, 0.2)), 0.5, 4.0)
    orbitals = scatter_about(seeds[5], (NB, NORB), 1.0, 6.0, ((0, 64),), jnp.float32)
    return {"density_matrix": density_matrix, "block_pattern": block_pattern, "tile_lists": tile_lists, "basis_values": basis_values, "core_density": core_density, "orbitals": orbitals}


pbe_kappa = 0.804
pbe_mu = 0.2195149727645171
exch_const = 0.75 * (3.0 / 3.141592653589793) ** (1.0 / 3.0)
grad_scale = 4.0 * (3.0 * 3.141592653589793 ** 2) ** (2.0 / 3.0)
density_floor = 0.2
spacing = 0.125

def energy(density, grad_square):
    scaled = grad_square / (grad_scale * density ** (8.0 / 3.0))
    enhance = 1.0 + pbe_kappa - pbe_kappa / (1.0 + pbe_mu * scaled / pbe_kappa)
    return -exch_const * density ** (4.0 / 3.0) * enhance

def total_energy(density, grad_square):
    return jnp.sum(energy(density, grad_square))

def centered(grid_values, direction):
    return (jnp.roll(grid_values, -1, direction) - jnp.roll(grid_values, 1, direction)) / (2.0 * spacing)

def potential(density):
    gradients = [centered(density, direction) for direction in range(3)]
    grad_square = gradients[0] * gradients[0] + gradients[1] * gradients[1] + gradients[2] * gradients[2]
    first, second = jax.grad(total_energy, argnums=(0, 1))(density, grad_square)
    divergence = jnp.zeros_like(density)
    for direction in range(3):
        divergence = divergence + centered(2.0 * second * gradients[direction], direction)
    return first - divergence

def reference(density_matrix, block_pattern, tile_lists, basis_values, core_density, orbitals):
    keep_mask = block_pattern.astype(jnp.bfloat16)
    masked = density_matrix.reshape(NBLK, BS, NBLK, BS) * keep_mask[:, None, :, None]
    tile_phi = basis_values.reshape(DEVICES, OV, CELLS)

    def tile_density(inputs):
        listed, phi_tile = inputs
        picked = jnp.take(masked, listed, axis=0)
        local_matrix = jnp.take(picked, listed, axis=2).reshape(OV, OV)
        product = jnp.dot(local_matrix, phi_tile, preferred_element_type=jnp.float32)
        return lax.optimization_barrier(jnp.sum(phi_tile.astype(jnp.float32) * product, axis=0))
    rho_tiles = lax.map(tile_density, (tile_lists, tile_phi))
    rho_grid = rho_tiles.reshape(N_ROW, N_COL, N_GZ, TX, TY, TZ).transpose(0, 3, 1, 4, 2, 5).reshape(NX, NY, NZ)
    density = jnp.maximum(rho_grid + core_density, density_floor)
    field = potential(density)
    field_tiles = field.reshape(N_ROW, TX, N_COL, TY, N_GZ, TZ).transpose(0, 2, 4, 1, 3, 5).reshape(DEVICES, CELLS)

    def add_tile(total, inputs):
        listed, phi_tile, tile_field = inputs
        weighted = (phi_tile.astype(jnp.float32) * tile_field[None, :]).astype(jnp.bfloat16)
        local_ham = lax.dot_general(weighted, phi_tile, (((1,), (1,)), ((), ())), preferred_element_type=jnp.float32)
        local_ham = local_ham.reshape(TL, BS, TL, BS).transpose(0, 2, 1, 3)
        total = total.at[listed[:, None], listed[None, :]].add(local_ham)
        return (total, None)
    start = jnp.zeros((NBLK, NBLK, BS, BS), jnp.float32)
    summed, unused = lax.scan(add_tile, start, (tile_lists, tile_phi, field_tiles))
    summed = summed * block_pattern.astype(jnp.float32)[:, :, None, None]
    hamiltonian = summed.transpose(0, 2, 1, 3).reshape(NB, NB)
    applied = jnp.dot(hamiltonian, orbitals, precision=lax.Precision.HIGHEST, preferred_element_type=jnp.float32)
    return (hamiltonian, applied)
```

```python
import jax
import jax.numpy as jnp
from jax import lax
from jax.experimental import pallas as pl
from jax.experimental.pallas import tpu as pltpu
from jax.sharding import PartitionSpec as P


pbe_kappa = 0.804
pbe_mu = 0.2195149727645171
exch_const = 0.75 * (3.0 / 3.141592653589793) ** (1.0 / 3.0)
grad_scale = 4.0 * (3.0 * 3.141592653589793**2) ** (2.0 / 3.0)
density_floor = 0.2
spacing = 0.125

PLANE = ("row", "col")
BS = 64
PAGES = 20
SCALE_ROWS = 32


def with_halo(cells, sides, width):
    for axis, dim in sides:
        count = lax.axis_size(axis)
        head = lax.slice_in_dim(cells, 0, width, axis=dim)
        tail = lax.slice_in_dim(cells, cells.shape[dim] - width, cells.shape[dim], axis=dim)
        cells = jnp.concatenate(
            [
                lax.ppermute(tail, axis, [(i, (i + 1) % count) for i in range(count)]),
                cells,
                lax.ppermute(head, axis, [((i + 1) % count, i) for i in range(count)]),
            ],
            axis=dim,
        )
    return cells


def energy(density, grad_square):
    scaled = grad_square / (grad_scale * density ** (8.0 / 3.0))
    enhance = 1.0 + pbe_kappa - pbe_kappa / (1.0 + pbe_mu * scaled / pbe_kappa)
    return -exch_const * density ** (4.0 / 3.0) * enhance


def total_energy(density, grad_square):
    return jnp.sum(energy(density, grad_square))


def centered(grid_values, direction):
    higher = [slice(1, -1), slice(1, -1), slice(1, -1)]
    lesser = [slice(1, -1), slice(1, -1), slice(1, -1)]
    higher[direction] = slice(2, None)
    lesser[direction] = slice(None, -2)
    return (grid_values[tuple(higher)] - grid_values[tuple(lesser)]) / (2.0 * spacing)


def potential_deep(density):
    padded = with_halo(density, (("row", 0), ("col", 1), ("gz", 2)), 2)
    gradients = [centered(padded, direction) for direction in range(3)]
    grad_square = (
        gradients[0] * gradients[0] + gradients[1] * gradients[1] + gradients[2] * gradients[2]
    )
    inner = padded[1:-1, 1:-1, 1:-1]
    first, second = jax.grad(total_energy, argnums=(0, 1))(inner, grad_square)
    divergence = centered(2.0 * second * gradients[0], 0)
    divergence = divergence + centered(2.0 * second * gradients[1], 1)
    divergence = divergence + centered(2.0 * second * gradients[2], 2)
    return first[1:-1, 1:-1, 1:-1] - divergence


def listed_pair(ids_ref, lists_ref, t):
    row, col, depth = ids_ref[0], ids_ref[1], ids_ref[2]
    tile = t * 4 + depth
    a0 = lists_ref[2 * row, tile] - 16 * row
    a1 = lists_ref[2 * row + 1, tile] - 16 * row
    b = lists_ref[col, tile] - 8 * col
    return a0, a1, b


def lane_pair(low, high, rows):
    lane = lax.broadcasted_iota(jnp.int32, (rows, 128), 1)
    return jnp.where(lane < BS, low, high)


def pack_kernel(ids_ref, lists_ref, pattern_ref, matrix_ref, out_ref, held):
    def turn(q, carry):
        rows = pl.ds(pl.multiple_of(q * 128, 128), 128)
        for m in range(4):
            block = matrix_ref[rows, 128 * m : 128 * m + 128].T
            for half in range(2):
                b = 2 * m + half
                keep = lane_pair(
                    pattern_ref[b, 2 * q].astype(jnp.float32),
                    pattern_ref[b, 2 * q + 1].astype(jnp.float32),
                    BS,
                ).astype(jnp.bfloat16)
                kept = block[BS * half : BS * half + BS] * keep
                held[0, b, q] = kept
                held[1, b, q] = pltpu.roll(kept, BS, 1)
        return carry

    lax.fori_loop(0, 8, turn, 0)

    def fill(t, carry):
        a0, a1, b = listed_pair(ids_ref, lists_ref, t)
        out_ref[t, :, 0:BS] = held[a0 & 1, b, a0 >> 1, :, 0:BS]
        out_ref[t, :, BS:128] = held[1 - (a1 & 1), b, a1 >> 1, :, BS:128]
        return carry

    lax.fori_loop(0, 128, fill, 0, unroll=4)


def density_kernel(blocks_ref, phi_ref, unit_ref, orbitals_ref, out_ref):
    phi = phi_ref[...]

    def part(n, total):
        rows = pl.ds(pl.multiple_of(n * 128, 128), 128)
        left = jnp.concatenate([blocks_ref[r, rows, :] for r in range(8)], axis=1)
        product = jnp.dot(left, phi, preferred_element_type=jnp.float32)
        return total + jnp.sum(phi_ref[rows, :].astype(jnp.float32) * product, axis=0, keepdims=True)

    out_ref[...] = lax.fori_loop(0, 8, part, jnp.zeros((1, 384), jnp.float32))


def ham_kernel(scale_ref, phi_ref, field_ref, out_ref):
    phi = phi_ref[...]

    def part(r, carry):
        rows = phi_ref[pl.ds(pl.multiple_of(r * 128, 128), 128), :].astype(jnp.float32)
        weighted = (rows * field_ref[...]).astype(jnp.bfloat16)
        block = lax.dot_general(phi, weighted, (((1,), (1,)), ((), ())), preferred_element_type=jnp.float32)
        out_ref[r] = block * scale_ref[0]
        return carry

    lax.fori_loop(0, 8, part, 0)


def coded(page):
    largest = jnp.max(jnp.abs(page), axis=0, keepdims=True)
    power = jnp.floor(jnp.log2(jnp.maximum(largest, 1e-30))) + 1.0
    power = jnp.clip(power, -90.0, 90.0)
    levels = jnp.clip(jnp.round(page * jnp.exp2(15.0 - power)), -32767.0, 32767.0)
    return levels.astype(jnp.int32).astype(jnp.int16), power


def owner_kernel(
    ids_ref, lists_ref, pattern_ref, scale_ref, blocks_ref, orbitals_ref, out_ref, sums, turned, terms, powers
):
    sums[...] = jnp.zeros_like(sums)

    def add(t, carry):
        a0, a1, b = listed_pair(ids_ref, lists_ref, t)
        block = blocks_ref[t]
        sums[a0 & 1, b, a0 >> 1, :, 0:BS] += block[:, 0:BS]
        sums[1 - (a1 & 1), b, a1 >> 1, :, BS:128] += block[:, BS:128]
        return carry

    lax.fori_loop(0, 128, add, 0, unroll=4)
    powers[...] = jnp.zeros_like(powers)

    def finish(q, carry):
        for b in range(8):
            keep = lane_pair(
                pattern_ref[b, 2 * q].astype(jnp.float32), pattern_ref[b, 2 * q + 1].astype(jnp.float32), BS
            )
            page = (sums[0, b, q] + pltpu.roll(sums[1, b, q], BS, 1)) * (keep * scale_ref[0])
            from_here = lax.rem(ids_ref[2] - b // 2 + 4, 4)
            start = pl.multiple_of(128 * from_here + BS * (b % 2), BS)
            turned[pl.ds(start, BS), :] = page
            levels, power = coded(page)
            place = (b % 2) * 8 + q
            out_ref[b // 2, pl.ds(pl.multiple_of(place * BS, BS), BS), :] = levels
            powers[b // 2, pl.ds(place, 1), :] = power
        part = lax.dot_general(
            turned[...],
            orbitals_ref[...].reshape(512, 128),
            (((0,), (0,)), ((), ())),
            precision=lax.Precision.HIGHEST,
            preferred_element_type=jnp.float32,
        )
        for half in range(2):
            for g in range(4):
                start = BS * half + 16 * g
                rows = pl.ds(pl.multiple_of((2 * q + half) * 16, 16), 16)
                terms[g, rows, :] = part[start : start + 16]
        return carry

    lax.fori_loop(0, 8, finish, 0)
    for g in range(4):
        for n in range(4):
            levels, power = coded(terms[g, BS * n : BS * n + BS, :])
            out_ref[g, (16 + n) * BS : (17 + n) * BS, :] = levels
            powers[g, 16 + n : 17 + n, :] = power
        out_ref[g, PAGES * BS : PAGES * BS + SCALE_ROWS, :] = (
            powers[g].astype(jnp.int32).astype(jnp.int16)
        )


def term_kernel(coded_ref, out_ref):
    steps = [
        jnp.exp2(coded_ref[g, PAGES * BS : PAGES * BS + SCALE_ROWS, :].astype(jnp.float32) - 15.0)
        for g in range(4)
    ]
    for n in range(4):
        total = jnp.zeros((BS, 128), jnp.float32)
        for g in range(4):
            levels = coded_ref[g, (16 + n) * BS : (17 + n) * BS, :].astype(jnp.float32)
            total = total + levels * steps[g][16 + n : 17 + n]
        out_ref[BS * n : BS * n + BS, :] = total


def share_kernel(coded_ref, out_ref):
    steps = [
        jnp.exp2(coded_ref[g, PAGES * BS : PAGES * BS + SCALE_ROWS, :].astype(jnp.float32) - 15.0)
        for g in range(4)
    ]
    for q in range(8):
        halves = []
        for half in range(2):
            place = half * 8 + q
            total = jnp.zeros((BS, 128), jnp.float32)
            for g in range(4):
                levels = coded_ref[g, place * BS : place * BS + BS, :].astype(jnp.float32)
                total = total + levels * steps[g][place : place + 1]
            halves.append(total)
        out_ref[128 * q : 128 * q + 128, :] = jnp.concatenate(halves, axis=0).T


smem = pl.BlockSpec(memory_space=pltpu.SMEM)
vmem = pl.BlockSpec(memory_space=pltpu.VMEM)
anywhere = pl.BlockSpec(memory_space=pl.ANY)


def exchange(array, axes):
    return lax.all_to_all(array, axes, 0, 0, tiled=True)


def shards(density_matrix, block_pattern, tile_lists, basis_values, core_density, orbitals):
    ids = jnp.stack([lax.axis_index("row"), lax.axis_index("col"), lax.axis_index("gz")]).astype(jnp.int32)
    lists = tile_lists.T
    pattern = block_pattern.T
    phi = basis_values.reshape(1024, 384)

    outgoing = pl.pallas_call(
        pack_kernel,
        out_shape=jax.ShapeDtypeStruct((128, BS, 128), jnp.bfloat16),
        in_specs=[smem, smem, smem, vmem],
        out_specs=vmem,
        scratch_shapes=[pltpu.VMEM((2, 8, 8, BS, 128), jnp.bfloat16)],
        name="pack",
    )(ids, lists, pattern, density_matrix)
    incoming = exchange(outgoing, PLANE)

    largest = jnp.full((8, 128), jnp.max(jnp.abs(phi)).astype(jnp.float32))
    for axis in PLANE:
        count = lax.axis_size(axis)
        step = 1
        while step < count:
            other = lax.ppermute(largest, axis, [(i, i ^ step) for i in range(count)])
            largest = jnp.maximum(largest, other)
            step *= 2
    columns = [orbitals]
    for step in range(1, 4):
        columns.append(lax.ppermute(orbitals, "gz", [(i, (i + step) % 4) for i in range(4)]))
    all_orbitals = jnp.stack(columns)
    unit = jnp.square(jnp.maximum(largest, 1e-15))[0, 0:1]

    rho = pl.pallas_call(
        density_kernel,
        out_shape=jax.ShapeDtypeStruct((1, 384), jnp.float32),
        in_specs=[vmem, vmem, anywhere, anywhere],
        out_specs=vmem,
        name="density",
    )(incoming.reshape(8, 1024, 128), phi, unit, all_orbitals)
    density = jnp.maximum(rho.reshape(core_density.shape) + core_density, density_floor)
    field = potential_deep(density)

    local_ham = pl.pallas_call(
        ham_kernel,
        out_shape=jax.ShapeDtypeStruct((8, 1024, 128), jnp.float32),
        in_specs=[smem, vmem, vmem],
        out_specs=vmem,
        name="ham",
    )(1.0 / unit, phi, field.reshape(1, -1))
    returning = local_ham.astype(jnp.float16).reshape(128, BS, 128)
    arrived = exchange(returning, PLANE).astype(jnp.float32)

    levels = pl.pallas_call(
        owner_kernel,
        out_shape=jax.ShapeDtypeStruct((4, PAGES * BS + SCALE_ROWS, 128), jnp.int16),
        in_specs=[smem, smem, smem, smem, vmem, vmem],
        out_specs=vmem,
        scratch_shapes=[
            pltpu.VMEM((2, 8, 8, BS, 128), jnp.float32),
            pltpu.VMEM((512, 128), jnp.float32),
            pltpu.VMEM((4, 256, 128), jnp.float32),
            pltpu.VMEM((4, SCALE_ROWS, 128), jnp.float32),
        ],
        name="owner",
    )(ids, lists, pattern, unit, arrived, all_orbitals)
    levels = exchange(levels, "gz")
    terms = pl.pallas_call(
        term_kernel,
        out_shape=jax.ShapeDtypeStruct((256, 128), jnp.float32),
        in_specs=[vmem],
        out_specs=vmem,
        name="terms",
    )(levels)
    applied = jnp.sum(exchange(terms.reshape(16, 16, 128), "col"), axis=0)
    share = pl.pallas_call(
        share_kernel,
        out_shape=jax.ShapeDtypeStruct((1024, 128), jnp.float32),
        in_specs=[vmem],
        out_specs=vmem,
        name="share",
    )(levels)
    return (share, applied)


def solution(mesh):
    placed = (
        P("row", "col"),
        P("row", "col"),
        P(),
        P("row", "col", "gz", None, None),
        P("row", "col", "gz"),
        P(("col", "gz"), None),
    )
    return jax.shard_map(
        shards,
        mesh=mesh,
        in_specs=placed,
        out_specs=(P("row", ("col", "gz")), P(("row", "col", "gz"), None)),
        check_vma=False,
    )
```

```python
import jax
import jax.numpy as jnp
from jax import lax
from jax.experimental import pallas as pl
from jax.experimental.pallas import tpu as pltpu
from jax.sharding import PartitionSpec as P


pbe_kappa = 0.804
pbe_mu = 0.2195149727645171
exch_const = 0.75 * (3.0 / 3.141592653589793) ** (1.0 / 3.0)
grad_scale = 4.0 * (3.0 * 3.141592653589793**2) ** (2.0 / 3.0)
density_floor = 0.2
spacing = 0.125


PLANE = ("row", "col")
BS = 64
MIB = 1024 * 1024
PAGES = 16
SCALES = 16


def with_halo(cells, sides, width):
    for axis, dim in sides:
        count = lax.axis_size(axis)
        head = lax.slice_in_dim(cells, 0, width, axis=dim)
        tail = lax.slice_in_dim(cells, cells.shape[dim] - width, cells.shape[dim], axis=dim)
        cells = jnp.concatenate(
            [
                lax.ppermute(tail, axis, [(i, (i + 1) % count) for i in range(count)]),
                cells,
                lax.ppermute(head, axis, [((i + 1) % count, i) for i in range(count)]),
            ],
            axis=dim,
        )
    return cells


def energy(density, grad_square):
    scaled = grad_square / (grad_scale * density ** (8.0 / 3.0))
    enhance = 1.0 + pbe_kappa - pbe_kappa / (1.0 + pbe_mu * scaled / pbe_kappa)
    return -exch_const * density ** (4.0 / 3.0) * enhance


def total_energy(density, grad_square):
    return jnp.sum(energy(density, grad_square))


def centered(grid_values, direction):
    higher = [slice(1, -1), slice(1, -1), slice(1, -1)]
    lesser = [slice(1, -1), slice(1, -1), slice(1, -1)]
    higher[direction] = slice(2, None)
    lesser[direction] = slice(None, -2)
    return (grid_values[tuple(higher)] - grid_values[tuple(lesser)]) / (2.0 * spacing)


def potential_deep(density):
    padded = with_halo(density, (("row", 0), ("col", 1), ("gz", 2)), 2)
    gradients = [centered(padded, direction) for direction in range(3)]
    grad_square = (
        gradients[0] * gradients[0] + gradients[1] * gradients[1] + gradients[2] * gradients[2]
    )
    inner = padded[1:-1, 1:-1, 1:-1]
    first, second = jax.grad(total_energy, argnums=(0, 1))(inner, grad_square)
    divergence = centered(2.0 * second * gradients[0], 0)
    divergence = divergence + centered(2.0 * second * gradients[1], 1)
    divergence = divergence + centered(2.0 * second * gradients[2], 2)
    return first[1:-1, 1:-1, 1:-1] - divergence


def listed_pair(ids_ref, lists_ref, t):
    row, col, depth = ids_ref[0], ids_ref[1], ids_ref[2]
    tile = t * 4 + depth
    a0 = lists_ref[2 * row, tile] - 16 * row
    a1 = lists_ref[2 * row + 1, tile] - 16 * row
    b = lists_ref[col, tile] - 8 * col
    return a0, a1, b


def lane_pair(low, high, rows):
    lane = lax.broadcasted_iota(jnp.int32, (rows, 128), 1)
    return jnp.where(lane < BS, low, high)


def pack_kernel(ids_ref, lists_ref, pattern_ref, matrix_ref, out_ref, held):
    def turn(q, carry):
        rows = pl.ds(pl.multiple_of(q * 128, 128), 128)
        for m in range(4):
            block = matrix_ref[rows, 128 * m : 128 * m + 128].T
            for half in range(2):
                b = 2 * m + half
                keep = lane_pair(
                    pattern_ref[b, 2 * q].astype(jnp.float32),
                    pattern_ref[b, 2 * q + 1].astype(jnp.float32),
                    BS,
                ).astype(jnp.bfloat16)
                kept = block[BS * half : BS * half + BS] * keep
                held[0, b, q] = kept
                held[1, b, q] = pltpu.roll(kept, BS, 1)
        return carry

    lax.fori_loop(0, 8, turn, 0)

    def fill(t, carry):
        a0, a1, b = listed_pair(ids_ref, lists_ref, t)
        out_ref[t, :, 0:BS] = held[a0 & 1, b, a0 >> 1, :, 0:BS]
        out_ref[t, :, BS:128] = held[1 - (a1 & 1), b, a1 >> 1, :, BS:128]
        return carry

    lax.fori_loop(0, 128, fill, 0, unroll=4)


def density_kernel(blocks_ref, phi_ref, unit_ref, orbitals_ref, out_ref):
    phi = phi_ref[...]

    def part(n, total):
        rows = pl.ds(pl.multiple_of(n * 128, 128), 128)
        left = jnp.concatenate([blocks_ref[r, rows, :] for r in range(8)], axis=1)
        product = jnp.dot(left, phi, preferred_element_type=jnp.float32)
        return total + jnp.sum(phi_ref[rows, :].astype(jnp.float32) * product, axis=0, keepdims=True)

    out_ref[...] = lax.fori_loop(0, 8, part, jnp.zeros((1, 384), jnp.float32))


def ham_kernel(scale_ref, phi_ref, field_ref, out_ref):
    phi = phi_ref[...]

    def part(r, carry):
        rows = phi_ref[pl.ds(pl.multiple_of(r * 128, 128), 128), :].astype(jnp.float32)
        weighted = (rows * field_ref[...]).astype(jnp.bfloat16)
        block = lax.dot_general(phi, weighted, (((1,), (1,)), ((), ())), preferred_element_type=jnp.float32)
        out_ref[r] = block * scale_ref[0]
        return carry

    lax.fori_loop(0, 8, part, 0)


def coded(page):
    largest = jnp.max(jnp.abs(page), axis=0, keepdims=True)
    power = jnp.floor(jnp.log2(jnp.maximum(largest, 1e-30))) + 1.0
    power = jnp.clip(power, -90.0, 90.0)
    levels = jnp.clip(jnp.round(page * jnp.exp2(15.0 - power)), -32767.0, 32767.0)
    return levels.astype(jnp.int32).astype(jnp.int16), power


def owner_kernel(
    ids_ref,
    lists_ref,
    pattern_ref,
    scale_ref,
    blocks_ref,
    orbitals_ref,
    terms_ref,
    out0_ref,
    out1_ref,
    out2_ref,
    out3_ref,
    sums,
    turned,
    powers,
):
    sums[...] = jnp.zeros_like(sums)

    def add(t, carry):
        a0, a1, b = listed_pair(ids_ref, lists_ref, t)
        block = blocks_ref[t]
        sums[a0 & 1, b, a0 >> 1, :, 0:BS] += block[:, 0:BS]
        sums[1 - (a1 & 1), b, a1 >> 1, :, BS:128] += block[:, BS:128]
        return carry

    lax.fori_loop(0, 128, add, 0, unroll=4)
    unit = scale_ref[0]
    outs = (out0_ref, out1_ref, out2_ref, out3_ref)

    def finish(q, carry):
        for n, out in enumerate(outs):
            peer = lax.rem(ids_ref[2] + n, 4)
            for half in range(2):
                b = 2 * peer + half
                keep = lane_pair(
                    pattern_ref[b, 2 * q].astype(jnp.float32), pattern_ref[b, 2 * q + 1].astype(jnp.float32), BS
                )
                page = (sums[0, b, q] + pltpu.roll(sums[1, b, q], BS, 1)) * (keep * unit)
                place = 2 * n + half
                turned[BS * place : BS * place + BS, :] = page
                levels, power = coded(page)
                place = half * 8 + q
                out[pl.ds(pl.multiple_of(place * BS, BS), BS), :] = levels
                powers[n, pl.ds(place, 1), :] = power
        part = lax.dot_general(
            turned[...],
            orbitals_ref[...].reshape(512, 128),
            (((0,), (0,)), ((), ())),
            precision=lax.Precision.HIGHEST,
            preferred_element_type=jnp.float32,
        )
        for half in range(2):
            levels, power = coded(part[BS * half : BS * half + BS])
            terms_ref[2 * q + half, 0:BS, :] = levels
            terms_ref[2 * q + half, BS : BS + 8, :] = (
                jnp.broadcast_to(power, (8, 128)).astype(jnp.int32).astype(jnp.int16)
            )
        return carry

    lax.fori_loop(0, 8, finish, 0)
    for n, out in enumerate(outs):
        out[PAGES * BS : PAGES * BS + SCALES, :] = powers[n].astype(jnp.int32).astype(jnp.int16)


def term_kernel(coded_ref, out_ref):
    total = jnp.zeros((BS, 128), jnp.float32)
    for c in range(16):
        step = jnp.exp2(coded_ref[c, BS : BS + 8, :].astype(jnp.float32)[0:1] - 15.0)
        total = total + coded_ref[c, 0:BS, :].astype(jnp.float32) * step
    out_ref[...] = total


def share_kernel(coded0_ref, coded1_ref, coded2_ref, coded3_ref, out_ref):
    parts = (coded0_ref, coded1_ref, coded2_ref, coded3_ref)
    steps = [jnp.exp2(part[PAGES * BS : PAGES * BS + SCALES, :].astype(jnp.float32) - 15.0) for part in parts]
    for q in range(8):
        halves = []
        for half in range(2):
            place = half * 8 + q
            total = jnp.zeros((BS, 128), jnp.float32)
            for part, step in zip(parts, steps):
                levels = part[place * BS : place * BS + BS, :].astype(jnp.float32)
                total = total + levels * step[place : place + 1]
            halves.append(total)
        out_ref[128 * q : 128 * q + 128, :] = jnp.concatenate(halves, axis=0).T


smem = pl.BlockSpec(memory_space=pltpu.SMEM)
vmem = pl.BlockSpec(memory_space=pltpu.VMEM)
anywhere = pl.BlockSpec(memory_space=pl.ANY)


def exchange(array, axes):
    return lax.all_to_all(array, axes, 0, 0, tiled=True)


def shards(density_matrix, block_pattern, tile_lists, basis_values, core_density, orbitals):
    ids = jnp.stack([lax.axis_index("row"), lax.axis_index("col"), lax.axis_index("gz")]).astype(jnp.int32)
    lists = tile_lists.T
    pattern = block_pattern.T
    phi = basis_values.reshape(1024, 384)

    outgoing = pl.pallas_call(
        pack_kernel,
        out_shape=jax.ShapeDtypeStruct((128, BS, 128), jnp.bfloat16),
        in_specs=[smem, smem, smem, vmem],
        out_specs=vmem,
        scratch_shapes=[pltpu.VMEM((2, 8, 8, BS, 128), jnp.bfloat16)],
        name="pack",
    )(ids, lists, pattern, density_matrix)
    incoming = exchange(outgoing, PLANE)

    largest = jnp.full((8, 128), jnp.max(jnp.abs(phi)).astype(jnp.float32))
    for step in (1, 2, 4):
        other = lax.ppermute(largest, "row", [(i, i ^ step) for i in range(8)])
        largest = jnp.maximum(largest, other)
    others = []
    for step in range(1, 16):
        others.append(lax.ppermute(largest, "col", [(i, i ^ step) for i in range(16)]))
    for other in others:
        largest = jnp.maximum(largest, other)
    columns = [orbitals]
    for step in range(1, 4):
        columns.append(lax.ppermute(orbitals, "gz", [(i, (i - step) % 4) for i in range(4)]))
    all_orbitals = jnp.stack(columns)
    unit = jnp.square(jnp.maximum(largest, 1e-15))[0, 0:1]

    rho = pl.pallas_call(
        density_kernel,
        out_shape=jax.ShapeDtypeStruct((1, 384), jnp.float32),
        in_specs=[vmem, vmem, anywhere, anywhere],
        out_specs=vmem,
        compiler_params=pltpu.CompilerParams(vmem_limit_bytes=12 * MIB),
        name="density",
    )(incoming.reshape(8, 1024, 128), phi, unit, all_orbitals)
    density = jnp.maximum(rho.reshape(core_density.shape) + core_density, density_floor)
    field = potential_deep(density)

    local_ham = pl.pallas_call(
        ham_kernel,
        out_shape=jax.ShapeDtypeStruct((8, 1024, 128), jnp.float32),
        in_specs=[smem, vmem, vmem],
        out_specs=vmem,
        compiler_params=pltpu.CompilerParams(vmem_limit_bytes=16 * MIB),
        name="ham",
    )(1.0 / unit, phi, field.reshape(1, -1))
    returning = local_ham.astype(jnp.float16).reshape(128, BS, 128)
    arrived = exchange(returning, PLANE).astype(jnp.float32)

    page_shape = jax.ShapeDtypeStruct((PAGES * BS + SCALES, 128), jnp.int16)
    terms, *pages = pl.pallas_call(
        owner_kernel,
        out_shape=[jax.ShapeDtypeStruct((16, BS + 8, 128), jnp.int16)] + [page_shape] * 4,
        in_specs=[smem, smem, smem, smem, vmem, vmem],
        out_specs=[vmem] * 5,
        scratch_shapes=[
            pltpu.VMEM((2, 8, 8, BS, 128), jnp.float32),
            pltpu.VMEM((512, 128), jnp.float32),
            pltpu.VMEM((4, SCALES, 128), jnp.float32),
        ],
        compiler_params=pltpu.CompilerParams(vmem_limit_bytes=24 * MIB),
        name="owner",
    )(ids, lists, pattern, unit, arrived, all_orbitals)
    terms = exchange(terms, "col")
    for step in range(1, 4):
        pages[step] = lax.ppermute(pages[step], "gz", [(i, (i + step) % 4) for i in range(4)])
    share = pl.pallas_call(
        share_kernel,
        out_shape=jax.ShapeDtypeStruct((1024, 128), jnp.float32),
        in_specs=[vmem] * 4,
        out_specs=vmem,
        compiler_params=pltpu.CompilerParams(vmem_limit_bytes=8 * MIB),
        name="share",
    )(*pages)
    sums = pl.pallas_call(
        term_kernel,
        out_shape=jax.ShapeDtypeStruct((BS, 128), jnp.float32),
        in_specs=[vmem],
        out_specs=vmem,
        compiler_params=pltpu.CompilerParams(vmem_limit_bytes=4 * MIB),
        name="sums",
    )(terms)
    applied = jnp.sum(exchange(sums.reshape(4, 16, 128), "gz"), axis=0)
    return (share, applied)


def solution(mesh):
    placed = (
        P("row", "col"),
        P("row", "col"),
        P(),
        P("row", "col", "gz", None, None),
        P("row", "col", "gz"),
        P(("col", "gz"), None),
    )
    return jax.shard_map(
        shards,
        mesh=mesh,
        in_specs=placed,
        out_specs=(P("row", ("col", "gz")), P(("row", "col", "gz"), None)),
        check_vma=False,
    )
```

```python
import jax
import jax.numpy as jnp
from jax import lax
from jax.experimental import pallas as pl
from jax.experimental.pallas import tpu as pltpu
from jax.sharding import PartitionSpec as P


pbe_kappa = 0.804
pbe_mu = 0.2195149727645171
exch_const = 0.75 * (3.0 / 3.141592653589793) ** (1.0 / 3.0)
grad_scale = 4.0 * (3.0 * 3.141592653589793**2) ** (2.0 / 3.0)
density_floor = 0.2
spacing = 0.125


PLANE = ("row", "col")
BS = 64
MIB = 1024 * 1024
PAGES = 16
SCALES = 16


def with_halo(cells, sides, width):
    for axis, dim in sides:
        count = lax.axis_size(axis)
        head = lax.slice_in_dim(cells, 0, width, axis=dim)
        tail = lax.slice_in_dim(cells, cells.shape[dim] - width, cells.shape[dim], axis=dim)
        cells = jnp.concatenate(
            [
                lax.ppermute(tail, axis, [(i, (i + 1) % count) for i in range(count)]),
                cells,
                lax.ppermute(head, axis, [((i + 1) % count, i) for i in range(count)]),
            ],
            axis=dim,
        )
    return cells


def energy(density, grad_square):
    scaled = grad_square / (grad_scale * density ** (8.0 / 3.0))
    enhance = 1.0 + pbe_kappa - pbe_kappa / (1.0 + pbe_mu * scaled / pbe_kappa)
    return -exch_const * density ** (4.0 / 3.0) * enhance


def total_energy(density, grad_square):
    return jnp.sum(energy(density, grad_square))


def centered(grid_values, direction):
    higher = [slice(1, -1), slice(1, -1), slice(1, -1)]
    lesser = [slice(1, -1), slice(1, -1), slice(1, -1)]
    higher[direction] = slice(2, None)
    lesser[direction] = slice(None, -2)
    return (grid_values[tuple(higher)] - grid_values[tuple(lesser)]) / (2.0 * spacing)


def potential_deep(density):
    padded = with_halo(density, (("row", 0), ("col", 1), ("gz", 2)), 2)
    gradients = [centered(padded, direction) for direction in range(3)]
    grad_square = (
        gradients[0] * gradients[0] + gradients[1] * gradients[1] + gradients[2] * gradients[2]
    )
    inner = padded[1:-1, 1:-1, 1:-1]
    first, second = jax.grad(total_energy, argnums=(0, 1))(inner, grad_square)
    divergence = centered(2.0 * second * gradients[0], 0)
    divergence = divergence + centered(2.0 * second * gradients[1], 1)
    divergence = divergence + centered(2.0 * second * gradients[2], 2)
    return first[1:-1, 1:-1, 1:-1] - divergence


def listed_pair(ids_ref, lists_ref, t):
    row, col, depth = ids_ref[0], ids_ref[1], ids_ref[2]
    tile = t * 4 + depth
    a0 = lists_ref[2 * row, tile] - 16 * row
    a1 = lists_ref[2 * row + 1, tile] - 16 * row
    b = lists_ref[col, tile] - 8 * col
    return a0, a1, b


def lane_pair(low, high, rows):
    lane = lax.broadcasted_iota(jnp.int32, (rows, 128), 1)
    return jnp.where(lane < BS, low, high)


def pack_kernel(ids_ref, lists_ref, pattern_ref, matrix_ref, out_ref, held):
    def turn(q, carry):
        rows = pl.ds(pl.multiple_of(q * 128, 128), 128)
        for m in range(4):
            block = matrix_ref[rows, 128 * m : 128 * m + 128].T
            for half in range(2):
                b = 2 * m + half
                keep = lane_pair(
                    pattern_ref[b, 2 * q].astype(jnp.float32),
                    pattern_ref[b, 2 * q + 1].astype(jnp.float32),
                    BS,
                ).astype(jnp.bfloat16)
                kept = block[BS * half : BS * half + BS] * keep
                held[0, b, q] = kept
                held[1, b, q] = pltpu.roll(kept, BS, 1)
        return carry

    lax.fori_loop(0, 8, turn, 0)

    def fill(t, carry):
        a0, a1, b = listed_pair(ids_ref, lists_ref, t)
        out_ref[t, :, 0:BS] = held[a0 & 1, b, a0 >> 1, :, 0:BS]
        out_ref[t, :, BS:128] = held[1 - (a1 & 1), b, a1 >> 1, :, BS:128]
        return carry

    lax.fori_loop(0, 128, fill, 0, unroll=4)


def density_kernel(blocks_ref, phi_ref, unit_ref, out_ref):
    phi = phi_ref[...]

    def part(n, total):
        rows = pl.ds(pl.multiple_of(n * 128, 128), 128)
        left = jnp.concatenate([blocks_ref[r, rows, :] for r in range(8)], axis=1)
        product = jnp.dot(left, phi, preferred_element_type=jnp.float32)
        return total + jnp.sum(phi_ref[rows, :].astype(jnp.float32) * product, axis=0, keepdims=True)

    out_ref[...] = lax.fori_loop(0, 8, part, jnp.zeros((1, 384), jnp.float32))


def ham_kernel(scale_ref, phi_ref, field_ref, out_ref):
    phi = phi_ref[...]

    def part(r, carry):
        rows = phi_ref[pl.ds(pl.multiple_of(r * 128, 128), 128), :].astype(jnp.float32)
        weighted = (rows * field_ref[...]).astype(jnp.bfloat16)
        block = lax.dot_general(phi, weighted, (((1,), (1,)), ((), ())), preferred_element_type=jnp.float32)
        out_ref[r] = block * scale_ref[0]
        return carry

    lax.fori_loop(0, 8, part, 0)


def coded(page):
    largest = jnp.max(jnp.abs(page), axis=0, keepdims=True)
    power = jnp.floor(jnp.log2(jnp.maximum(largest, 1e-30))) + 1.0
    power = jnp.clip(power, -90.0, 90.0)
    levels = jnp.clip(jnp.round(page * jnp.exp2(15.0 - power)), -32767.0, 32767.0)
    return levels.astype(jnp.int32).astype(jnp.int16), power


def owner_kernel(
    ids_ref,
    lists_ref,
    pattern_ref,
    scale_ref,
    blocks_ref,
    orbitals_ref,
    terms_ref,
    out0_ref,
    out1_ref,
    out2_ref,
    out3_ref,
    sums,
    turned,
    powers,
    products,
):
    sums[...] = jnp.zeros_like(sums)

    def add(t, carry):
        a0, a1, b = listed_pair(ids_ref, lists_ref, t)
        block = blocks_ref[t] * scale_ref[8 * (((t & 15) ^ ids_ref[1]) >> 2)]
        sums[a0 & 1, b, a0 >> 1, :, 0:BS] += block[:, 0:BS]
        sums[1 - (a1 & 1), b, a1 >> 1, :, BS:128] += block[:, BS:128]
        return carry

    lax.fori_loop(0, 128, add, 0, unroll=4)
    outs = (out0_ref, out1_ref, out2_ref, out3_ref)

    def finish(q, carry):
        for n, out in enumerate(outs):
            peer = lax.rem(ids_ref[2] + n, 4)
            for half in range(2):
                b = 2 * peer + half
                keep = lane_pair(
                    pattern_ref[b, 2 * q].astype(jnp.float32), pattern_ref[b, 2 * q + 1].astype(jnp.float32), BS
                )
                page = (sums[0, b, q] + pltpu.roll(sums[1, b, q], BS, 1)) * keep
                place = 2 * n + half
                turned[BS * place : BS * place + BS, :] = page
                levels, power = coded(page)
                place = half * 8 + q
                out[pl.ds(pl.multiple_of(place * BS, BS), BS), :] = levels
                powers[n, pl.ds(place, 1), :] = power
        part = lax.dot_general(
            turned[...],
            orbitals_ref[...].reshape(512, 128),
            (((0,), (0,)), ((), ())),
            precision=lax.Precision.HIGHEST,
            preferred_element_type=jnp.float32,
        )
        for half in range(2):
            for g in range(4):
                start = BS * half + 16 * g
                rows = pl.ds(pl.multiple_of((2 * q + half) * 16, 16), 16)
                products[g, rows, :] = part[start : start + 16]
        return carry

    lax.fori_loop(0, 8, finish, 0)
    for g in range(4):
        product_powers = []
        for n in range(4):
            levels, power = coded(products[g, BS * n : BS * n + BS, :])
            terms_ref[g, BS * n : BS * n + BS, :] = levels
            product_powers.append(power)
        terms_ref[g, 4 * BS : 4 * BS + 8, :] = (
            jnp.concatenate(product_powers * 2, axis=0).astype(jnp.int32).astype(jnp.int16)
        )
    for n, out in enumerate(outs):
        out[PAGES * BS : PAGES * BS + SCALES, :] = powers[n].astype(jnp.int32).astype(jnp.int16)


def term_kernel(coded_ref, out_ref):
    steps = [
        jnp.exp2(coded_ref[g, 4 * BS : 4 * BS + 8, :].astype(jnp.float32) - 15.0) for g in range(4)
    ]
    for n in range(4):
        total = jnp.zeros((BS, 128), jnp.float32)
        for g in range(4):
            levels = coded_ref[g, BS * n : BS * n + BS, :].astype(jnp.float32)
            total = total + levels * steps[g][n : n + 1]
        out_ref[BS * n : BS * n + BS, :] = total


def share_kernel(coded0_ref, coded1_ref, coded2_ref, coded3_ref, out_ref):
    parts = (coded0_ref, coded1_ref, coded2_ref, coded3_ref)
    steps = [jnp.exp2(part[PAGES * BS : PAGES * BS + SCALES, :].astype(jnp.float32) - 15.0) for part in parts]
    for q in range(8):
        halves = []
        for half in range(2):
            place = half * 8 + q
            total = jnp.zeros((BS, 128), jnp.float32)
            for part, step in zip(parts, steps):
                levels = part[place * BS : place * BS + BS, :].astype(jnp.float32)
                total = total + levels * step[place : place + 1]
            halves.append(total)
        out_ref[128 * q : 128 * q + 128, :] = jnp.concatenate(halves, axis=0).T


smem = pl.BlockSpec(memory_space=pltpu.SMEM)
vmem = pl.BlockSpec(memory_space=pltpu.VMEM)
anywhere = pl.BlockSpec(memory_space=pl.ANY)


def exchange(array, axes):
    return lax.all_to_all(array, axes, 0, 0, tiled=True)


def shards(density_matrix, block_pattern, tile_lists, basis_values, core_density, orbitals):
    ids = jnp.stack([lax.axis_index("row"), lax.axis_index("col"), lax.axis_index("gz")]).astype(jnp.int32)
    lists = tile_lists.T
    pattern = block_pattern.T
    phi = basis_values.reshape(1024, 384)

    outgoing = pl.pallas_call(
        pack_kernel,
        out_shape=jax.ShapeDtypeStruct((128, BS, 128), jnp.bfloat16),
        in_specs=[smem, smem, smem, vmem],
        out_specs=vmem,
        scratch_shapes=[pltpu.VMEM((2, 8, 8, BS, 128), jnp.bfloat16)],
        name="pack",
    )(ids, lists, pattern, density_matrix)
    incoming = exchange(outgoing, PLANE)

    largest = jnp.full((8, 128), jnp.max(jnp.abs(phi)).astype(jnp.float32))
    for step in (1, 2, 4):
        other = lax.ppermute(largest, "row", [(i, i ^ step) for i in range(8)])
        largest = jnp.maximum(largest, other)
    others = []
    for step in (1, 2, 3):
        others.append(lax.ppermute(largest, "col", [(i, i ^ step) for i in range(16)]))
    for other in others:
        largest = jnp.maximum(largest, other)
    largest = jnp.maximum(largest, 1e-15)
    unit = jnp.square(largest)[0, 0:1]

    rho = pl.pallas_call(
        density_kernel,
        out_shape=jax.ShapeDtypeStruct((1, 384), jnp.float32),
        in_specs=[vmem, vmem, anywhere],
        out_specs=vmem,
        compiler_params=pltpu.CompilerParams(vmem_limit_bytes=12 * MIB),
        name="density",
    )(incoming.reshape(8, 1024, 128), phi, unit)
    density = jnp.maximum(rho.reshape(core_density.shape) + core_density, density_floor)
    field = potential_deep(density)

    local_ham = pl.pallas_call(
        ham_kernel,
        out_shape=jax.ShapeDtypeStruct((8, 1024, 128), jnp.float32),
        in_specs=[smem, vmem, vmem],
        out_specs=vmem,
        compiler_params=pltpu.CompilerParams(vmem_limit_bytes=16 * MIB),
        name="ham",
    )(1.0 / unit, phi, field.reshape(1, -1))
    returning = local_ham.astype(jnp.float16).reshape(128, BS, 128)
    arrived = exchange(returning, PLANE).astype(jnp.float32)
    peaks = [largest]
    for step in (4, 8, 12):
        peaks.append(lax.ppermute(largest, "col", [(i, i ^ step) for i in range(16)]))
    columns = [orbitals]
    for step in range(1, 4):
        columns.append(lax.ppermute(orbitals, "gz", [(i, (i - step) % 4) for i in range(4)]))
    units = jnp.square(jnp.concatenate(peaks, axis=0)[:, 0])
    all_orbitals = jnp.stack(columns)

    page_shape = jax.ShapeDtypeStruct((PAGES * BS + SCALES, 128), jnp.int16)
    terms, *pages = pl.pallas_call(
        owner_kernel,
        out_shape=[jax.ShapeDtypeStruct((4, 4 * BS + 8, 128), jnp.int16)] + [page_shape] * 4,
        in_specs=[smem, smem, smem, smem, vmem, vmem],
        out_specs=[vmem] * 5,
        scratch_shapes=[
            pltpu.VMEM((2, 8, 8, BS, 128), jnp.float32),
            pltpu.VMEM((512, 128), jnp.float32),
            pltpu.VMEM((4, SCALES, 128), jnp.float32),
            pltpu.VMEM((4, 256, 128), jnp.float32),
        ],
        compiler_params=pltpu.CompilerParams(vmem_limit_bytes=24 * MIB),
        name="owner",
    )(ids, lists, pattern, units, arrived, all_orbitals)
    terms = exchange(terms, "gz")
    for step in range(1, 4):
        pages[step] = lax.ppermute(pages[step], "gz", [(i, (i + step) % 4) for i in range(4)])
    sums = pl.pallas_call(
        term_kernel,
        out_shape=jax.ShapeDtypeStruct((256, 128), jnp.float32),
        in_specs=[vmem],
        out_specs=vmem,
        compiler_params=pltpu.CompilerParams(vmem_limit_bytes=4 * MIB),
        name="sums",
    )(terms)
    applied = jnp.sum(exchange(sums.reshape(16, 16, 128), "col"), axis=0)
    share = pl.pallas_call(
        share_kernel,
        out_shape=jax.ShapeDtypeStruct((1024, 128), jnp.float32),
        in_specs=[vmem] * 4,
        out_specs=vmem,
        compiler_params=pltpu.CompilerParams(vmem_limit_bytes=8 * MIB),
        name="share",
    )(*pages)
    return (share, applied)


def solution(mesh):
    placed = (
        P("row", "col"),
        P("row", "col"),
        P(),
        P("row", "col", "gz", None, None),
        P("row", "col", "gz"),
        P(("col", "gz"), None),
    )
    return jax.shard_map(
        shards,
        mesh=mesh,
        in_specs=placed,
        out_specs=(P("row", ("col", "gz")), P(("row", "col", "gz"), None)),
        check_vma=False,
    )
```

```python
import jax
import jax.numpy as jnp
from jax import lax
from jax.experimental import pallas as pl
from jax.experimental.pallas import tpu as pltpu
from jax.sharding import PartitionSpec as P


pbe_kappa = 0.804
pbe_mu = 0.2195149727645171
exch_const = 0.75 * (3.0 / 3.141592653589793) ** (1.0 / 3.0)
grad_scale = 4.0 * (3.0 * 3.141592653589793**2) ** (2.0 / 3.0)
density_floor = 0.2
spacing = 0.125


PLANE = ("row", "col")
BS = 64
MIB = 1024 * 1024
PAGES = 16
SCALES = 16
LEVELS = 32760.0


def with_halo(cells, sides, width):
    for axis, dim in sides:
        count = lax.axis_size(axis)
        head = lax.slice_in_dim(cells, 0, width, axis=dim)
        tail = lax.slice_in_dim(cells, cells.shape[dim] - width, cells.shape[dim], axis=dim)
        cells = jnp.concatenate(
            [
                lax.ppermute(tail, axis, [(i, (i + 1) % count) for i in range(count)]),
                cells,
                lax.ppermute(head, axis, [((i + 1) % count, i) for i in range(count)]),
            ],
            axis=dim,
        )
    return cells


def energy(density, grad_square):
    scaled = grad_square / (grad_scale * density ** (8.0 / 3.0))
    enhance = 1.0 + pbe_kappa - pbe_kappa / (1.0 + pbe_mu * scaled / pbe_kappa)
    return -exch_const * density ** (4.0 / 3.0) * enhance


def total_energy(density, grad_square):
    return jnp.sum(energy(density, grad_square))


def centered(grid_values, direction):
    higher = [slice(1, -1), slice(1, -1), slice(1, -1)]
    lesser = [slice(1, -1), slice(1, -1), slice(1, -1)]
    higher[direction] = slice(2, None)
    lesser[direction] = slice(None, -2)
    return (grid_values[tuple(higher)] - grid_values[tuple(lesser)]) / (2.0 * spacing)


def potential_deep(density):
    padded = with_halo(density, (("row", 0), ("col", 1), ("gz", 2)), 2)
    gradients = [centered(padded, direction) for direction in range(3)]
    grad_square = (
        gradients[0] * gradients[0] + gradients[1] * gradients[1] + gradients[2] * gradients[2]
    )
    inner = padded[1:-1, 1:-1, 1:-1]
    first, second = jax.grad(total_energy, argnums=(0, 1))(inner, grad_square)
    divergence = centered(2.0 * second * gradients[0], 0)
    divergence = divergence + centered(2.0 * second * gradients[1], 1)
    divergence = divergence + centered(2.0 * second * gradients[2], 2)
    return first[1:-1, 1:-1, 1:-1] - divergence


def listed_pair(ids_ref, lists_ref, t):
    row, col, depth = ids_ref[0], ids_ref[1], ids_ref[2]
    tile = t * 4 + depth
    a0 = lists_ref[2 * row, tile] - 16 * row
    a1 = lists_ref[2 * row + 1, tile] - 16 * row
    b = lists_ref[col, tile] - 8 * col
    return a0, a1, b


def lane_pair(low, high, rows):
    lane = lax.broadcasted_iota(jnp.int32, (rows, 128), 1)
    return jnp.where(lane < BS, low, high)


def pack_kernel(ids_ref, lists_ref, pattern_ref, matrix_ref, out_ref, pages_ref, held):
    def turn(q, carry):
        rows = pl.ds(pl.multiple_of(q * 128, 128), 128)
        first = (q < 4).astype(jnp.float32)
        for m in range(4):
            block = matrix_ref[rows, 128 * m : 128 * m + 128].T
            for half in range(2):
                b = 2 * m + half
                low = pattern_ref[b, 2 * q].astype(jnp.float32)
                high = pattern_ref[b, 2 * q + 1].astype(jnp.float32)
                part = block[BS * half : BS * half + BS]
                straight = lane_pair(low * first, high * (1.0 - first), BS).astype(jnp.bfloat16)
                crossed = lane_pair(low * (1.0 - first), high * first, BS).astype(jnp.bfloat16)
                held[b * 8 + q] = part * straight
                held[64 + b * 8 + q] = pltpu.roll(part * crossed, BS, 1)
        return carry

    lax.fori_loop(0, 8, turn, 0)

    def fill(t, carry):
        a0, a1, b = listed_pair(ids_ref, lists_ref, t)
        page0 = (a0 & 1) * 64 + b * 8 + (a0 >> 1)
        page1 = (1 - (a1 & 1)) * 64 + b * 8 + (a1 >> 1)
        pages_ref[t] = page0
        pages_ref[128 + t] = page1
        out_ref[t] = held[page0] + held[page1]
        return carry

    lax.fori_loop(0, 128, fill, 0, unroll=4)


def density_kernel(blocks_ref, phi_ref, unit_ref, out_ref):
    def part(n, total):
        rows = pl.ds(pl.multiple_of(n * 256, 256), 256)
        left = jnp.concatenate([blocks_ref[r, rows, :] for r in range(8)], axis=1)
        product = jnp.dot(left, phi_ref[...], preferred_element_type=jnp.float32)
        return total + jnp.sum(phi_ref[rows, :].astype(jnp.float32) * product, axis=0, keepdims=True)

    out_ref[...] = lax.fori_loop(0, 4, part, jnp.zeros((1, 384), jnp.float32))


def ham_kernel(scale_ref, phi_ref, field_ref, out_ref):
    def part(r, carry):
        rows = phi_ref[pl.ds(pl.multiple_of(r * 256, 256), 256), :].astype(jnp.float32)
        weighted = (rows * field_ref[...]).astype(jnp.bfloat16)
        block = lax.dot_general(
            phi_ref[...], weighted, (((1,), (1,)), ((), ())), preferred_element_type=jnp.float32
        )
        out_ref[2 * r] = block[:, 0:128] * scale_ref[0]
        out_ref[2 * r + 1] = block[:, 128:256] * scale_ref[0]
        return carry

    lax.fori_loop(0, 4, part, 0)


def coded(page):
    largest = jnp.max(jnp.abs(page), axis=0, keepdims=True)
    power = jnp.floor(jnp.log2(jnp.clip(largest, 1e-27, 1e27))) + 1.0
    levels = jnp.round(page * (jnp.exp2(-power) * LEVELS))
    return levels.astype(jnp.int32).astype(jnp.int16), power


def step_of(power):
    return jnp.exp2(power.astype(jnp.float32)) * (1.0 / LEVELS)


def owner_kernel(
    ids_ref,
    pages_ref,
    pattern_ref,
    scale_ref,
    blocks_ref,
    orbitals_ref,
    terms_ref,
    out0_ref,
    out1_ref,
    out2_ref,
    out3_ref,
    sums,
    factors,
    turned,
    powers,
    products,
):
    sums[...] = jnp.zeros_like(sums)

    def add(t, carry):
        page0, page1 = pages_ref[t], pages_ref[128 + t]
        block = blocks_ref[t] * scale_ref[8 * (((t & 15) ^ ids_ref[1]) >> 2)]
        sums[page0] += block
        sums[page1] += block
        return carry

    lax.fori_loop(0, 128, add, 0, unroll=4)
    outs = (out0_ref, out1_ref, out2_ref, out3_ref)

    orbitals = orbitals_ref[...]
    orbitals_high = orbitals.astype(jnp.bfloat16)
    orbitals_low = (orbitals - orbitals_high.astype(jnp.float32)).astype(jnp.bfloat16)
    factors[...] = jnp.concatenate([orbitals_high, orbitals_high, orbitals_low], axis=1)

    def finish(q, carry):
        first = (q < 4).astype(jnp.float32)
        for n, out in enumerate(outs):
            peer = lax.rem(ids_ref[2] + n, 4)
            for half in range(2):
                b = 2 * peer + half
                low = pattern_ref[b, 2 * q].astype(jnp.float32)
                high = pattern_ref[b, 2 * q + 1].astype(jnp.float32)
                straight = lane_pair(low * first, high * (1.0 - first), BS)
                crossed = lane_pair(high * first, low * (1.0 - first), BS)
                page = sums[b * 8 + q] * straight + pltpu.roll(sums[64 + b * 8 + q] * crossed, BS, 1)
                page_high = page.astype(jnp.bfloat16)
                page_low = (page - page_high.astype(jnp.float32)).astype(jnp.bfloat16)
                place = 2 * n + half
                turned[BS * place : BS * place + BS, :] = page_high
                turned[512 + BS * place : 512 + BS * place + BS, :] = page_low
                turned[1024 + BS * place : 1024 + BS * place + BS, :] = page_high
                levels, power = coded(page)
                place = half * 8 + q
                out[pl.ds(pl.multiple_of(place * BS, BS), BS), :] = levels
                powers[n, pl.ds(place, 1), :] = power
        part = jnp.dot(factors[...], turned[...], preferred_element_type=jnp.float32).T
        for half in range(2):
            for g in range(4):
                start = BS * half + 16 * g
                rows = pl.ds(pl.multiple_of((2 * q + half) * 16, 16), 16)
                products[g, rows, :] = part[start : start + 16]
        return carry

    lax.fori_loop(0, 8, finish, 0)
    for g in range(4):
        product_powers = []
        for n in range(4):
            levels, power = coded(products[g, BS * n : BS * n + BS, :])
            terms_ref[g, BS * n : BS * n + BS, :] = levels
            product_powers.append(power)
        terms_ref[g, 4 * BS : 4 * BS + 8, :] = (
            jnp.concatenate(product_powers * 2, axis=0).astype(jnp.int32).astype(jnp.int16)
        )
    for n, out in enumerate(outs):
        out[PAGES * BS : PAGES * BS + SCALES, :] = powers[n].astype(jnp.int32).astype(jnp.int16)


def term_kernel(coded_ref, out_ref):
    steps = [
        step_of(coded_ref[g, 4 * BS : 4 * BS + 8, :]) for g in range(4)
    ]
    for n in range(4):
        total = jnp.zeros((BS, 128), jnp.float32)
        for g in range(4):
            levels = coded_ref[g, BS * n : BS * n + BS, :].astype(jnp.float32)
            total = total + levels * steps[g][n : n + 1]
        out_ref[BS * n : BS * n + BS, :] = total


def share_kernel(coded0_ref, coded1_ref, coded2_ref, coded3_ref, out_ref):
    parts = (coded0_ref, coded1_ref, coded2_ref, coded3_ref)
    steps = [step_of(part[PAGES * BS : PAGES * BS + SCALES, :]) for part in parts]
    for q in range(8):
        halves = []
        for half in range(2):
            place = half * 8 + q
            total = jnp.zeros((BS, 128), jnp.float32)
            for part, step in zip(parts, steps):
                levels = part[place * BS : place * BS + BS, :].astype(jnp.float32)
                total = total + levels * step[place : place + 1]
            halves.append(total)
        out_ref[128 * q : 128 * q + 128, :] = jnp.concatenate(halves, axis=0).T


smem = pl.BlockSpec(memory_space=pltpu.SMEM)
vmem = pl.BlockSpec(memory_space=pltpu.VMEM)
anywhere = pl.BlockSpec(memory_space=pl.ANY)


def exchange(array, axes):
    return lax.all_to_all(array, axes, 0, 0, tiled=True)


def shards(density_matrix, block_pattern, tile_lists, basis_values, core_density, orbitals):
    ids = jnp.stack([lax.axis_index("row"), lax.axis_index("col"), lax.axis_index("gz")]).astype(jnp.int32)
    lists = tile_lists.T
    pattern = block_pattern.T
    phi = basis_values.reshape(1024, 384)

    outgoing, page_table = pl.pallas_call(
        pack_kernel,
        out_shape=[
            jax.ShapeDtypeStruct((128, BS, 128), jnp.bfloat16),
            jax.ShapeDtypeStruct((256,), jnp.int32),
        ],
        in_specs=[smem, smem, smem, vmem],
        out_specs=[vmem, smem],
        scratch_shapes=[pltpu.VMEM((128, BS, 128), jnp.bfloat16)],
        name="pack",
    )(ids, lists, pattern, density_matrix)
    incoming = exchange(outgoing, PLANE)

    largest = jnp.full((8, 128), jnp.max(jnp.abs(phi)).astype(jnp.float32))
    for step in (1, 2, 4):
        other = lax.ppermute(largest, "row", [(i, i ^ step) for i in range(8)])
        largest = jnp.maximum(largest, other)
    others = []
    for step in (1, 2, 3):
        others.append(lax.ppermute(largest, "col", [(i, i ^ step) for i in range(16)]))
    for other in others:
        largest = jnp.maximum(largest, other)
    largest = jnp.maximum(largest, 1e-15)
    unit = jnp.square(largest)[0, 0:1]

    rho = pl.pallas_call(
        density_kernel,
        out_shape=jax.ShapeDtypeStruct((1, 384), jnp.float32),
        in_specs=[vmem, vmem, anywhere],
        out_specs=vmem,
        compiler_params=pltpu.CompilerParams(vmem_limit_bytes=12 * MIB),
        name="density",
    )(incoming.reshape(8, 1024, 128), phi, unit)
    density = jnp.maximum(rho.reshape(core_density.shape) + core_density, density_floor)
    field = potential_deep(density)

    local_ham = pl.pallas_call(
        ham_kernel,
        out_shape=jax.ShapeDtypeStruct((8, 1024, 128), jnp.float32),
        in_specs=[smem, vmem, vmem],
        out_specs=vmem,
        compiler_params=pltpu.CompilerParams(vmem_limit_bytes=16 * MIB),
        name="ham",
    )(1.0 / unit, phi, field.reshape(1, -1))
    returning = local_ham.astype(jnp.float16).reshape(128, BS, 128)
    arrived = exchange(returning, PLANE).astype(jnp.float32)
    peaks = [largest]
    for step in (4, 8, 12):
        peaks.append(lax.ppermute(largest, "col", [(i, i ^ step) for i in range(16)]))
    columns = [orbitals]
    for step in range(1, 4):
        columns.append(lax.ppermute(orbitals, "gz", [(i, (i - step) % 4) for i in range(4)]))
    units = jnp.square(jnp.concatenate(peaks, axis=0)[:, 0])
    all_orbitals = jnp.concatenate(columns, axis=0).T

    page_shape = jax.ShapeDtypeStruct((PAGES * BS + SCALES, 128), jnp.int16)
    terms, *pages = pl.pallas_call(
        owner_kernel,
        out_shape=[jax.ShapeDtypeStruct((4, 4 * BS + 8, 128), jnp.int16)] + [page_shape] * 4,
        in_specs=[smem, smem, smem, smem, vmem, vmem],
        out_specs=[vmem] * 5,
        scratch_shapes=[
            pltpu.VMEM((128, BS, 128), jnp.float32),
            pltpu.VMEM((128, 1536), jnp.bfloat16),
            pltpu.VMEM((1536, 128), jnp.bfloat16),
            pltpu.VMEM((4, SCALES, 128), jnp.float32),
            pltpu.VMEM((4, 256, 128), jnp.float32),
        ],
        compiler_params=pltpu.CompilerParams(vmem_limit_bytes=24 * MIB),
        name="owner",
    )(ids, page_table, pattern, units, arrived, all_orbitals)
    terms = exchange(terms, "gz")
    for step in range(1, 4):
        pages[step] = lax.ppermute(pages[step], "gz", [(i, (i + step) % 4) for i in range(4)])
    sums = pl.pallas_call(
        term_kernel,
        out_shape=jax.ShapeDtypeStruct((256, 128), jnp.float32),
        in_specs=[vmem],
        out_specs=vmem,
        compiler_params=pltpu.CompilerParams(vmem_limit_bytes=4 * MIB),
        name="sums",
    )(terms)
    applied = jnp.sum(exchange(sums.reshape(16, 16, 128), "col"), axis=0)
    share = pl.pallas_call(
        share_kernel,
        out_shape=jax.ShapeDtypeStruct((1024, 128), jnp.float32),
        in_specs=[vmem] * 4,
        out_specs=vmem,
        compiler_params=pltpu.CompilerParams(vmem_limit_bytes=8 * MIB),
        name="share",
    )(*pages)
    return (share, applied)


def solution(mesh):
    placed = (
        P("row", "col"),
        P("row", "col"),
        P(),
        P("row", "col", "gz", None, None),
        P("row", "col", "gz"),
        P(("col", "gz"), None),
    )
    return jax.shard_map(
        shards,
        mesh=mesh,
        in_specs=placed,
        out_specs=(P("row", ("col", "gz")), P(("row", "col", "gz"), None)),
        check_vma=False,
    )
```

```python
import jax
import jax.numpy as jnp
from jax import lax
from jax.experimental import pallas as pl
from jax.experimental.pallas import tpu as pltpu
from jax.sharding import PartitionSpec as P


pbe_kappa = 0.804
pbe_mu = 0.2195149727645171
exch_const = 0.75 * (3.0 / 3.141592653589793) ** (1.0 / 3.0)
grad_scale = 4.0 * (3.0 * 3.141592653589793**2) ** (2.0 / 3.0)
density_floor = 0.2
spacing = 0.125


PLANE = ("row", "col")
BS = 64
MIB = 1024 * 1024
PAGES = 16
SCALES = 16
LEVELS = 32760.0


def with_halo(cells, sides, width):
    for axis, dim in sides:
        count = lax.axis_size(axis)
        head = lax.slice_in_dim(cells, 0, width, axis=dim)
        tail = lax.slice_in_dim(cells, cells.shape[dim] - width, cells.shape[dim], axis=dim)
        cells = jnp.concatenate(
            [
                lax.ppermute(tail, axis, [(i, (i + 1) % count) for i in range(count)]),
                cells,
                lax.ppermute(head, axis, [((i + 1) % count, i) for i in range(count)]),
            ],
            axis=dim,
        )
    return cells


def energy(density, grad_square):
    scaled = grad_square / (grad_scale * density ** (8.0 / 3.0))
    enhance = 1.0 + pbe_kappa - pbe_kappa / (1.0 + pbe_mu * scaled / pbe_kappa)
    return -exch_const * density ** (4.0 / 3.0) * enhance


def total_energy(density, grad_square):
    return jnp.sum(energy(density, grad_square))


def centered(grid_values, direction):
    higher = [slice(1, -1), slice(1, -1), slice(1, -1)]
    lesser = [slice(1, -1), slice(1, -1), slice(1, -1)]
    higher[direction] = slice(2, None)
    lesser[direction] = slice(None, -2)
    return (grid_values[tuple(higher)] - grid_values[tuple(lesser)]) / (2.0 * spacing)


def potential_deep(slab):
    padded = with_halo(slab, (("col", 1),), 2)
    gradients = [centered(padded, direction) for direction in range(3)]
    grad_square = (
        gradients[0] * gradients[0] + gradients[1] * gradients[1] + gradients[2] * gradients[2]
    )
    inner = padded[1:-1, 1:-1, 1:-1]
    first, second = jax.grad(total_energy, argnums=(0, 1))(inner, grad_square)
    divergence = centered(2.0 * second * gradients[0], 0)
    divergence = divergence + centered(2.0 * second * gradients[1], 1)
    divergence = divergence + centered(2.0 * second * gradients[2], 2)
    return first[1:-1, 1:-1, 1:-1] - divergence


def listed_pair(ids_ref, lists_ref, t):
    row, col, depth = ids_ref[0], ids_ref[1], ids_ref[2]
    tile = t * 4 + depth
    a0 = lists_ref[2 * row, tile] - 16 * row
    a1 = lists_ref[2 * row + 1, tile] - 16 * row
    b = lists_ref[col, tile] - 8 * col
    return a0, a1, b


def lane_pair(low, high, rows):
    lane = lax.broadcasted_iota(jnp.int32, (rows, 128), 1)
    return jnp.where(lane < BS, low, high)


def pack_kernel(ids_ref, lists_ref, pattern_ref, matrix_ref, out_ref, pages_ref, held):
    def turn(q, carry):
        rows = pl.ds(pl.multiple_of(q * 128, 128), 128)
        first = (q < 4).astype(jnp.float32)
        for m in range(4):
            block = matrix_ref[rows, 128 * m : 128 * m + 128].T
            for half in range(2):
                b = 2 * m + half
                low = pattern_ref[b, 2 * q].astype(jnp.float32)
                high = pattern_ref[b, 2 * q + 1].astype(jnp.float32)
                part = block[BS * half : BS * half + BS]
                straight = lane_pair(low * first, high * (1.0 - first), BS).astype(jnp.bfloat16)
                crossed = lane_pair(low * (1.0 - first), high * first, BS).astype(jnp.bfloat16)
                held[b * 8 + q] = part * straight
                held[64 + b * 8 + q] = pltpu.roll(part * crossed, BS, 1)
        return carry

    lax.fori_loop(0, 8, turn, 0)

    def fill(t, carry):
        a0, a1, b = listed_pair(ids_ref, lists_ref, t)
        page0 = (a0 & 1) * 64 + b * 8 + (a0 >> 1)
        page1 = (1 - (a1 & 1)) * 64 + b * 8 + (a1 >> 1)
        pages_ref[t] = page0
        pages_ref[128 + t] = page1
        out_ref[t] = held[page0] + held[page1]
        return carry

    lax.fori_loop(0, 128, fill, 0, unroll=4)


def density_kernel(blocks_ref, phi_ref, core_ref, unit_ref, orbitals_ref, out_ref):
    def part(n, total):
        rows = pl.ds(pl.multiple_of(n * 256, 256), 256)
        left = jnp.concatenate([blocks_ref[r, rows, :] for r in range(8)], axis=1)
        product = jnp.dot(left, phi_ref[...], preferred_element_type=jnp.float32)
        return total + jnp.sum(phi_ref[rows, :].astype(jnp.float32) * product, axis=0, keepdims=True)

    rho = lax.fori_loop(0, 4, part, jnp.zeros((1, 384), jnp.float32))
    density = jnp.maximum(rho + core_ref[...], density_floor)
    out_ref[...] = jnp.broadcast_to(density[None], (32, 1, 384))


def slab_kernel(ids_ref, tiles_ref, out_ref):
    row, depth = ids_ref[0], ids_ref[2]
    line = lax.broadcasted_iota(jnp.int32, (16, 384), 0) * 24
    lane = lax.broadcasted_iota(jnp.int32, (16, 384), 1)
    own_line = (lane >= line) & (lane < line + 24)
    rows = []
    for across in (7, 0, 1):
        pieces = []
        for along in (3, 0, 1):
            place = lax.rem(row + across, 8) * 4 + lax.rem(depth + along, 4)
            pieces.append(jnp.where(own_line, jnp.broadcast_to(tiles_ref[place], (16, 384)), 0.0))
        rows.append(jnp.concatenate(pieces, axis=1))
    left = jnp.concatenate(rows, axis=0)
    source = lax.rem(lax.broadcasted_iota(jnp.int32, (1152, 128), 0), 24)
    piece = lax.broadcasted_iota(jnp.int32, (1152, 128), 0) // 384
    target = lax.broadcasted_iota(jnp.int32, (1152, 128), 1)
    wanted = source + 2 + 24 * (piece - 1)
    chosen = jnp.where((wanted == target) & (target < 28), 1.0, 0.0)
    slab = jnp.dot(left, chosen, precision=lax.Precision.HIGHEST, preferred_element_type=jnp.float32)
    out_ref[...] = slab.reshape(6, 8, 128)


def ham_kernel(scale_ref, phi_ref, field_ref, out_ref):
    def part(r, carry):
        rows = phi_ref[pl.ds(pl.multiple_of(r * 256, 256), 256), :].astype(jnp.float32)
        weighted = (rows * field_ref[...]).astype(jnp.bfloat16)
        block = lax.dot_general(
            phi_ref[...], weighted, (((1,), (1,)), ((), ())), preferred_element_type=jnp.float32
        )
        out_ref[2 * r] = block[:, 0:128] * scale_ref[0]
        out_ref[2 * r + 1] = block[:, 128:256] * scale_ref[0]
        return carry

    lax.fori_loop(0, 4, part, 0)


def coded(page):
    largest = jnp.max(jnp.abs(page), axis=0, keepdims=True)
    power = jnp.floor(jnp.log2(jnp.clip(largest, 1e-27, 1e27))) + 1.0
    levels = jnp.round(page * (jnp.exp2(-power) * LEVELS))
    return levels.astype(jnp.int32).astype(jnp.int16), power


def step_of(power):
    return jnp.exp2(power.astype(jnp.float32)) * (1.0 / LEVELS)


def owner_kernel(
    ids_ref,
    pages_ref,
    pattern_ref,
    scale_ref,
    blocks_ref,
    orbitals_ref,
    terms_ref,
    out0_ref,
    out1_ref,
    out2_ref,
    out3_ref,
    sums,
    factors,
    turned,
    powers,
    products,
):
    sums[...] = jnp.zeros_like(sums)

    def add(t, carry):
        page0, page1 = pages_ref[t], pages_ref[128 + t]
        block = blocks_ref[t] * scale_ref[8 * ((t & 15) ^ ids_ref[1])]
        sums[page0] += block
        sums[page1] += block
        return carry

    lax.fori_loop(0, 128, add, 0, unroll=4)
    outs = (out0_ref, out1_ref, out2_ref, out3_ref)

    orbitals = orbitals_ref[...]
    orbitals_high = orbitals.astype(jnp.bfloat16)
    orbitals_low = (orbitals - orbitals_high.astype(jnp.float32)).astype(jnp.bfloat16)
    factors[...] = jnp.concatenate([orbitals_high, orbitals_high, orbitals_low], axis=1)

    def finish(q, carry):
        first = (q < 4).astype(jnp.float32)
        for n, out in enumerate(outs):
            peer = lax.rem(ids_ref[2] + n, 4)
            for half in range(2):
                b = 2 * peer + half
                low = pattern_ref[b, 2 * q].astype(jnp.float32)
                high = pattern_ref[b, 2 * q + 1].astype(jnp.float32)
                straight = lane_pair(low * first, high * (1.0 - first), BS)
                crossed = lane_pair(high * first, low * (1.0 - first), BS)
                page = sums[b * 8 + q] * straight + pltpu.roll(sums[64 + b * 8 + q] * crossed, BS, 1)
                page_high = page.astype(jnp.bfloat16)
                page_low = (page - page_high.astype(jnp.float32)).astype(jnp.bfloat16)
                place = 2 * n + half
                turned[BS * place : BS * place + BS, :] = page_high
                turned[512 + BS * place : 512 + BS * place + BS, :] = page_low
                turned[1024 + BS * place : 1024 + BS * place + BS, :] = page_high
                levels, power = coded(page)
                place = half * 8 + q
                out[pl.ds(pl.multiple_of(place * BS, BS), BS), :] = levels
                powers[n, pl.ds(place, 1), :] = power
        part = jnp.dot(factors[...], turned[...], preferred_element_type=jnp.float32).T
        for half in range(2):
            for g in range(4):
                start = BS * half + 16 * g
                rows = pl.ds(pl.multiple_of((2 * q + half) * 16, 16), 16)
                products[g, rows, :] = part[start : start + 16]
        return carry

    lax.fori_loop(0, 8, finish, 0)
    for g in range(4):
        product_powers = []
        for n in range(4):
            levels, power = coded(products[g, BS * n : BS * n + BS, :])
            terms_ref[g, BS * n : BS * n + BS, :] = levels
            product_powers.append(power)
        terms_ref[g, 4 * BS : 4 * BS + 8, :] = (
            jnp.concatenate(product_powers * 2, axis=0).astype(jnp.int32).astype(jnp.int16)
        )
    for n, out in enumerate(outs):
        out[PAGES * BS : PAGES * BS + SCALES, :] = powers[n].astype(jnp.int32).astype(jnp.int16)


def term_kernel(coded_ref, out_ref):
    steps = [
        step_of(coded_ref[g, 4 * BS : 4 * BS + 8, :]) for g in range(4)
    ]
    for n in range(4):
        total = jnp.zeros((BS, 128), jnp.float32)
        for g in range(4):
            levels = coded_ref[g, BS * n : BS * n + BS, :].astype(jnp.float32)
            total = total + levels * steps[g][n : n + 1]
        out_ref[BS * n : BS * n + BS, :] = total


def share_kernel(coded0_ref, coded1_ref, coded2_ref, coded3_ref, out_ref):
    parts = (coded0_ref, coded1_ref, coded2_ref, coded3_ref)
    steps = [step_of(part[PAGES * BS : PAGES * BS + SCALES, :]) for part in parts]
    for q in range(8):
        halves = []
        for half in range(2):
            place = half * 8 + q
            total = jnp.zeros((BS, 128), jnp.float32)
            for part, step in zip(parts, steps):
                levels = part[place * BS : place * BS + BS, :].astype(jnp.float32)
                total = total + levels * step[place : place + 1]
            halves.append(total)
        out_ref[128 * q : 128 * q + 128, :] = jnp.concatenate(halves, axis=0).T


smem = pl.BlockSpec(memory_space=pltpu.SMEM)
vmem = pl.BlockSpec(memory_space=pltpu.VMEM)
anywhere = pl.BlockSpec(memory_space=pl.ANY)


def exchange(array, axes):
    return lax.all_to_all(array, axes, 0, 0, tiled=True)


def shards(density_matrix, block_pattern, tile_lists, basis_values, core_density, orbitals):
    ids = jnp.stack([lax.axis_index("row"), lax.axis_index("col"), lax.axis_index("gz")]).astype(jnp.int32)
    lists = tile_lists.T
    pattern = block_pattern.T
    phi = basis_values.reshape(1024, 384)

    outgoing, page_table = pl.pallas_call(
        pack_kernel,
        out_shape=[
            jax.ShapeDtypeStruct((128, BS, 128), jnp.bfloat16),
            jax.ShapeDtypeStruct((256,), jnp.int32),
        ],
        in_specs=[smem, smem, smem, vmem],
        out_specs=[vmem, smem],
        scratch_shapes=[pltpu.VMEM((128, BS, 128), jnp.bfloat16)],
        name="pack",
    )(ids, lists, pattern, density_matrix)
    incoming = exchange(outgoing, PLANE)

    largest = jnp.full((8, 128), jnp.max(jnp.abs(phi)).astype(jnp.float32))
    for step in (1, 2, 4):
        other = lax.ppermute(largest, "row", [(i, i ^ step) for i in range(8)])
        largest = jnp.maximum(largest, other)
    columns = [orbitals]
    for step in range(1, 4):
        columns.append(lax.ppermute(orbitals, "gz", [(i, (i - step) % 4) for i in range(4)]))
    all_orbitals = jnp.concatenate(columns, axis=0).T
    largest = jnp.maximum(largest, 1e-15)
    unit = jnp.square(largest)[0, 0:1]

    densities = pl.pallas_call(
        density_kernel,
        out_shape=jax.ShapeDtypeStruct((32, 1, 384), jnp.float32),
        in_specs=[vmem, vmem, vmem, anywhere, anywhere],
        out_specs=vmem,
        compiler_params=pltpu.CompilerParams(vmem_limit_bytes=12 * MIB),
        name="density",
    )(incoming.reshape(8, 1024, 128), phi, core_density.reshape(1, 384), unit, all_orbitals)
    slab = pl.pallas_call(
        slab_kernel,
        out_shape=jax.ShapeDtypeStruct((6, 8, 128), jnp.float32),
        in_specs=[smem, vmem],
        out_specs=vmem,
        compiler_params=pltpu.CompilerParams(vmem_limit_bytes=8 * MIB),
        name="slab",
    )(ids, exchange(densities, ("row", "gz")))
    field = potential_deep(slab[:, :, :28])

    local_ham = pl.pallas_call(
        ham_kernel,
        out_shape=jax.ShapeDtypeStruct((8, 1024, 128), jnp.float32),
        in_specs=[smem, vmem, vmem],
        out_specs=vmem,
        compiler_params=pltpu.CompilerParams(vmem_limit_bytes=16 * MIB),
        name="ham",
    )(1.0 / unit, phi, field.reshape(1, -1))
    returning = local_ham.astype(jnp.float16).reshape(128, BS, 128)
    arrived = exchange(returning, PLANE).astype(jnp.float32)
    peaks = [largest]
    for step in range(1, 16):
        peaks.append(lax.ppermute(largest, "col", [(i, i ^ step) for i in range(16)]))
    units = jnp.square(jnp.concatenate(peaks, axis=0)[:, 0])

    page_shape = jax.ShapeDtypeStruct((PAGES * BS + SCALES, 128), jnp.int16)
    terms, *pages = pl.pallas_call(
        owner_kernel,
        out_shape=[jax.ShapeDtypeStruct((4, 4 * BS + 8, 128), jnp.int16)] + [page_shape] * 4,
        in_specs=[smem, smem, smem, smem, vmem, vmem],
        out_specs=[vmem] * 5,
        scratch_shapes=[
            pltpu.VMEM((128, BS, 128), jnp.float32),
            pltpu.VMEM((128, 1536), jnp.bfloat16),
            pltpu.VMEM((1536, 128), jnp.bfloat16),
            pltpu.VMEM((4, SCALES, 128), jnp.float32),
            pltpu.VMEM((4, 256, 128), jnp.float32),
        ],
        compiler_params=pltpu.CompilerParams(vmem_limit_bytes=24 * MIB),
        name="owner",
    )(ids, page_table, pattern, units, arrived, all_orbitals)
    terms = exchange(terms, "gz")
    for step in range(1, 4):
        pages[step] = lax.ppermute(pages[step], "gz", [(i, (i + step) % 4) for i in range(4)])
    sums = pl.pallas_call(
        term_kernel,
        out_shape=jax.ShapeDtypeStruct((256, 128), jnp.float32),
        in_specs=[vmem],
        out_specs=vmem,
        compiler_params=pltpu.CompilerParams(vmem_limit_bytes=4 * MIB),
        name="sums",
    )(terms)
    applied = jnp.sum(exchange(sums.reshape(16, 16, 128), "col"), axis=0)
    share = pl.pallas_call(
        share_kernel,
        out_shape=jax.ShapeDtypeStruct((1024, 128), jnp.float32),
        in_specs=[vmem] * 4,
        out_specs=vmem,
        compiler_params=pltpu.CompilerParams(vmem_limit_bytes=8 * MIB),
        name="share",
    )(*pages)
    return (share, applied)


def solution(mesh):
    placed = (
        P("row", "col"),
        P("row", "col"),
        P(),
        P("row", "col", "gz", None, None),
        P("row", "col", "gz"),
        P(("col", "gz"), None),
    )
    return jax.shard_map(
        shards,
        mesh=mesh,
        in_specs=placed,
        out_specs=(P("row", ("col", "gz")), P(("row", "col", "gz"), None)),
        check_vma=False,
    )
```

```python
import jax
import jax.numpy as jnp
from jax import lax
from jax.experimental import pallas as pl
from jax.experimental.pallas import tpu as pltpu
from jax.sharding import PartitionSpec as P


pbe_kappa = 0.804
pbe_mu = 0.2195149727645171
exch_const = 0.75 * (3.0 / 3.141592653589793) ** (1.0 / 3.0)
grad_scale = 4.0 * (3.0 * 3.141592653589793**2) ** (2.0 / 3.0)
density_floor = 0.2
spacing = 0.125


PLANE = ("row", "col")
BS = 64
MIB = 1024 * 1024
PAGES = 16
SCALES = 16
LEVELS = 32760.0


def with_halo(cells, sides, width):
    for axis, dim in sides:
        count = lax.axis_size(axis)
        head = lax.slice_in_dim(cells, 0, width, axis=dim)
        tail = lax.slice_in_dim(cells, cells.shape[dim] - width, cells.shape[dim], axis=dim)
        cells = jnp.concatenate(
            [
                lax.ppermute(tail, axis, [(i, (i + 1) % count) for i in range(count)]),
                cells,
                lax.ppermute(head, axis, [((i + 1) % count, i) for i in range(count)]),
            ],
            axis=dim,
        )
    return cells


def energy(density, grad_square):
    scaled = grad_square / (grad_scale * density ** (8.0 / 3.0))
    enhance = 1.0 + pbe_kappa - pbe_kappa / (1.0 + pbe_mu * scaled / pbe_kappa)
    return -exch_const * density ** (4.0 / 3.0) * enhance


def total_energy(density, grad_square):
    return jnp.sum(energy(density, grad_square))


def centered(grid_values, direction):
    higher = [slice(1, -1), slice(1, -1), slice(1, -1)]
    lesser = [slice(1, -1), slice(1, -1), slice(1, -1)]
    higher[direction] = slice(2, None)
    lesser[direction] = slice(None, -2)
    return (grid_values[tuple(higher)] - grid_values[tuple(lesser)]) / (2.0 * spacing)


def potential_deep(slab):
    padded = with_halo(slab, (("col", 1),), 2)
    gradients = [centered(padded, direction) for direction in range(3)]
    grad_square = (
        gradients[0] * gradients[0] + gradients[1] * gradients[1] + gradients[2] * gradients[2]
    )
    inner = padded[1:-1, 1:-1, 1:-1]
    first, second = jax.grad(total_energy, argnums=(0, 1))(inner, grad_square)
    divergence = centered(2.0 * second * gradients[0], 0)
    divergence = divergence + centered(2.0 * second * gradients[1], 1)
    divergence = divergence + centered(2.0 * second * gradients[2], 2)
    return first[1:-1, 1:-1, 1:-1] - divergence


def listed_pair(ids_ref, lists_ref, t):
    row, col, depth = ids_ref[0], ids_ref[1], ids_ref[2]
    tile = t * 4 + depth
    a0 = lists_ref[2 * row, tile] - 16 * row
    a1 = lists_ref[2 * row + 1, tile] - 16 * row
    b = lists_ref[col, tile] - 8 * col
    return a0, a1, b


def lane_pair(low, high, rows):
    lane = lax.broadcasted_iota(jnp.int32, (rows, 128), 1)
    return jnp.where(lane < BS, low, high)


def pack_kernel(ids_ref, lists_ref, pattern_ref, matrix_ref, out_ref, pages_ref, held):
    def turn(q, carry):
        rows = pl.ds(pl.multiple_of(q * 128, 128), 128)
        first = (q < 4).astype(jnp.float32)
        for m in range(4):
            block = matrix_ref[rows, 128 * m : 128 * m + 128].T
            for half in range(2):
                b = 2 * m + half
                low = pattern_ref[b, 2 * q].astype(jnp.float32)
                high = pattern_ref[b, 2 * q + 1].astype(jnp.float32)
                part = block[BS * half : BS * half + BS]
                straight = lane_pair(low * first, high * (1.0 - first), BS).astype(jnp.bfloat16)
                crossed = lane_pair(low * (1.0 - first), high * first, BS).astype(jnp.bfloat16)
                held[b * 8 + q] = part * straight
                held[64 + b * 8 + q] = pltpu.roll(part * crossed, BS, 1)
        return carry

    lax.fori_loop(0, 8, turn, 0)

    def fill(t, carry):
        a0, a1, b = listed_pair(ids_ref, lists_ref, t)
        page0 = (a0 & 1) * 64 + b * 8 + (a0 >> 1)
        page1 = (1 - (a1 & 1)) * 64 + b * 8 + (a1 >> 1)
        pages_ref[t] = page0
        pages_ref[128 + t] = page1
        out_ref[t] = held[page0] + held[page1]
        return carry

    lax.fori_loop(0, 128, fill, 0, unroll=4)


def density_kernel(blocks_ref, phi_ref, core_ref, unit_ref, orbitals_ref, out_ref):
    def part(n, total):
        rows = pl.ds(pl.multiple_of(n * 256, 256), 256)
        left = jnp.concatenate([blocks_ref[r, rows, :] for r in range(8)], axis=1)
        product = jnp.dot(left, phi_ref[...], preferred_element_type=jnp.float32)
        return total + jnp.sum(phi_ref[rows, :].astype(jnp.float32) * product, axis=0, keepdims=True)

    rho = lax.fori_loop(0, 4, part, jnp.zeros((1, 384), jnp.float32))
    density = jnp.maximum(rho + core_ref[...], density_floor)
    out_ref[...] = jnp.broadcast_to(density[None], (32, 1, 384))


def slab_kernel(ids_ref, tiles_ref, out_ref):
    row, depth = ids_ref[0], ids_ref[2]
    line = lax.broadcasted_iota(jnp.int32, (16, 384), 0) * 24
    lane = lax.broadcasted_iota(jnp.int32, (16, 384), 1)
    own_line = (lane >= line) & (lane < line + 24)
    rows = []
    for across in (7, 0, 1):
        pieces = []
        for along in (3, 0, 1):
            place = lax.rem(row + across, 8) * 4 + lax.rem(depth + along, 4)
            pieces.append(jnp.where(own_line, jnp.broadcast_to(tiles_ref[place], (16, 384)), 0.0))
        rows.append(jnp.concatenate(pieces, axis=1))
    left = jnp.concatenate(rows, axis=0)
    source = lax.rem(lax.broadcasted_iota(jnp.int32, (1152, 128), 0), 24)
    piece = lax.broadcasted_iota(jnp.int32, (1152, 128), 0) // 384
    target = lax.broadcasted_iota(jnp.int32, (1152, 128), 1)
    wanted = source + 2 + 24 * (piece - 1)
    chosen = jnp.where((wanted == target) & (target < 28), 1.0, 0.0)
    slab = jnp.dot(left, chosen, precision=lax.Precision.HIGHEST, preferred_element_type=jnp.float32)
    out_ref[...] = slab.reshape(6, 8, 128)


def ham_kernel(scale_ref, phi_ref, field_ref, out_ref):
    def part(r, carry):
        rows = phi_ref[pl.ds(pl.multiple_of(r * 256, 256), 256), :].astype(jnp.float32)
        weighted = (rows * field_ref[...]).astype(jnp.bfloat16)
        block = lax.dot_general(
            phi_ref[...], weighted, (((1,), (1,)), ((), ())), preferred_element_type=jnp.float32
        )
        out_ref[2 * r] = block[:, 0:128] * scale_ref[0]
        out_ref[2 * r + 1] = block[:, 128:256] * scale_ref[0]
        return carry

    lax.fori_loop(0, 4, part, 0)


def coded(page):
    largest = jnp.max(jnp.abs(page), axis=0, keepdims=True)
    power = jnp.floor(jnp.log2(jnp.clip(largest, 1e-27, 1e27))) + 1.0
    levels = jnp.round(page * (jnp.exp2(-power) * LEVELS))
    return levels.astype(jnp.int32).astype(jnp.int16), power


def step_of(power):
    return jnp.exp2(power.astype(jnp.float32)) * (1.0 / LEVELS)


def owner_kernel(
    ids_ref,
    pages_ref,
    pattern_ref,
    scale_ref,
    blocks_ref,
    orbitals_ref,
    terms_ref,
    out0_ref,
    out1_ref,
    out2_ref,
    out3_ref,
    sums,
    factors,
    turned,
    powers,
    products,
):
    sums[...] = jnp.zeros_like(sums)

    def add(t, carry):
        page0, page1 = pages_ref[t], pages_ref[128 + t]
        block = blocks_ref[t] * scale_ref[8 * (((t & 15) ^ ids_ref[1]) >> 2)]
        sums[page0] += block
        sums[page1] += block
        return carry

    lax.fori_loop(0, 128, add, 0, unroll=4)
    outs = (out0_ref, out1_ref, out2_ref, out3_ref)

    orbitals = orbitals_ref[...]
    orbitals_high = orbitals.astype(jnp.bfloat16)
    orbitals_low = (orbitals - orbitals_high.astype(jnp.float32)).astype(jnp.bfloat16)
    factors[...] = jnp.concatenate([orbitals_high, orbitals_high, orbitals_low], axis=1)

    def finish(q, carry):
        first = (q < 4).astype(jnp.float32)
        for n, out in enumerate(outs):
            peer = lax.rem(ids_ref[2] + n, 4)
            for half in range(2):
                b = 2 * peer + half
                low = pattern_ref[b, 2 * q].astype(jnp.float32)
                high = pattern_ref[b, 2 * q + 1].astype(jnp.float32)
                straight = lane_pair(low * first, high * (1.0 - first), BS)
                crossed = lane_pair(high * first, low * (1.0 - first), BS)
                page = sums[b * 8 + q] * straight + pltpu.roll(sums[64 + b * 8 + q] * crossed, BS, 1)
                page_high = page.astype(jnp.bfloat16)
                page_low = (page - page_high.astype(jnp.float32)).astype(jnp.bfloat16)
                place = 2 * n + half
                turned[BS * place : BS * place + BS, :] = page_high
                turned[512 + BS * place : 512 + BS * place + BS, :] = page_low
                turned[1024 + BS * place : 1024 + BS * place + BS, :] = page_high
                levels, power = coded(page)
                place = half * 8 + q
                out[pl.ds(pl.multiple_of(place * BS, BS), BS), :] = levels
                powers[n, pl.ds(place, 1), :] = power
        part = jnp.dot(factors[...], turned[...], preferred_element_type=jnp.float32).T
        for half in range(2):
            for g in range(4):
                start = BS * half + 16 * g
                rows = pl.ds(pl.multiple_of((2 * q + half) * 16, 16), 16)
                products[g, rows, :] = part[start : start + 16]
        return carry

    lax.fori_loop(0, 8, finish, 0)
    for g in range(4):
        product_powers = []
        for n in range(4):
            levels, power = coded(products[g, BS * n : BS * n + BS, :])
            terms_ref[g, BS * n : BS * n + BS, :] = levels
            product_powers.append(power)
        terms_ref[g, 4 * BS : 4 * BS + 8, :] = (
            jnp.concatenate(product_powers * 2, axis=0).astype(jnp.int32).astype(jnp.int16)
        )
    for n, out in enumerate(outs):
        out[PAGES * BS : PAGES * BS + SCALES, :] = powers[n].astype(jnp.int32).astype(jnp.int16)


def term_kernel(coded_ref, out_ref):
    steps = [
        step_of(coded_ref[g, 4 * BS : 4 * BS + 8, :]) for g in range(4)
    ]
    for n in range(4):
        total = jnp.zeros((BS, 128), jnp.float32)
        for g in range(4):
            levels = coded_ref[g, BS * n : BS * n + BS, :].astype(jnp.float32)
            total = total + levels * steps[g][n : n + 1]
        out_ref[BS * n : BS * n + BS, :] = total


def share_kernel(coded0_ref, coded1_ref, coded2_ref, coded3_ref, out_ref):
    parts = (coded0_ref, coded1_ref, coded2_ref, coded3_ref)
    steps = [step_of(part[PAGES * BS : PAGES * BS + SCALES, :]) for part in parts]
    for q in range(8):
        halves = []
        for half in range(2):
            place = half * 8 + q
            total = jnp.zeros((BS, 128), jnp.float32)
            for part, step in zip(parts, steps):
                levels = part[place * BS : place * BS + BS, :].astype(jnp.float32)
                total = total + levels * step[place : place + 1]
            halves.append(total)
        out_ref[128 * q : 128 * q + 128, :] = jnp.concatenate(halves, axis=0).T


smem = pl.BlockSpec(memory_space=pltpu.SMEM)
vmem = pl.BlockSpec(memory_space=pltpu.VMEM)
anywhere = pl.BlockSpec(memory_space=pl.ANY)


def exchange(array, axes):
    return lax.all_to_all(array, axes, 0, 0, tiled=True)


def shards(density_matrix, block_pattern, tile_lists, basis_values, core_density, orbitals):
    ids = jnp.stack([lax.axis_index("row"), lax.axis_index("col"), lax.axis_index("gz")]).astype(jnp.int32)
    lists = tile_lists.T
    pattern = block_pattern.T
    phi = basis_values.reshape(1024, 384)

    outgoing, page_table = pl.pallas_call(
        pack_kernel,
        out_shape=[
            jax.ShapeDtypeStruct((128, BS, 128), jnp.bfloat16),
            jax.ShapeDtypeStruct((256,), jnp.int32),
        ],
        in_specs=[smem, smem, smem, vmem],
        out_specs=[vmem, smem],
        scratch_shapes=[pltpu.VMEM((128, BS, 128), jnp.bfloat16)],
        name="pack",
    )(ids, lists, pattern, density_matrix)
    incoming = exchange(outgoing, PLANE)

    largest = jnp.full((8, 128), jnp.max(jnp.abs(phi)).astype(jnp.float32))
    for step in (1, 2, 4):
        other = lax.ppermute(largest, "row", [(i, i ^ step) for i in range(8)])
        largest = jnp.maximum(largest, other)
    others = []
    for step in (1, 2, 3):
        others.append(lax.ppermute(largest, "col", [(i, i ^ step) for i in range(16)]))
    for other in others:
        largest = jnp.maximum(largest, other)
    columns = [orbitals]
    for step in range(1, 4):
        columns.append(lax.ppermute(orbitals, "gz", [(i, (i - step) % 4) for i in range(4)]))
    all_orbitals = jnp.concatenate(columns, axis=0).T
    largest = jnp.maximum(largest, 1e-15)
    unit = jnp.square(largest)[0, 0:1]

    densities = pl.pallas_call(
        density_kernel,
        out_shape=jax.ShapeDtypeStruct((32, 1, 384), jnp.float32),
        in_specs=[vmem, vmem, vmem, anywhere, anywhere],
        out_specs=vmem,
        compiler_params=pltpu.CompilerParams(vmem_limit_bytes=12 * MIB),
        name="density",
    )(incoming.reshape(8, 1024, 128), phi, core_density.reshape(1, 384), unit, all_orbitals)
    slab = pl.pallas_call(
        slab_kernel,
        out_shape=jax.ShapeDtypeStruct((6, 8, 128), jnp.float32),
        in_specs=[smem, vmem],
        out_specs=vmem,
        compiler_params=pltpu.CompilerParams(vmem_limit_bytes=8 * MIB),
        name="slab",
    )(ids, exchange(densities, ("row", "gz")))
    field = potential_deep(slab[:, :, :28])

    local_ham = pl.pallas_call(
        ham_kernel,
        out_shape=jax.ShapeDtypeStruct((8, 1024, 128), jnp.float32),
        in_specs=[smem, vmem, vmem],
        out_specs=vmem,
        compiler_params=pltpu.CompilerParams(vmem_limit_bytes=16 * MIB),
        name="ham",
    )(1.0 / unit, phi, field.reshape(1, -1))
    returning = local_ham.astype(jnp.float16).reshape(128, BS, 128)
    arrived = exchange(returning, PLANE).astype(jnp.float32)
    peaks = [largest]
    for step in (4, 8, 12):
        peaks.append(lax.ppermute(largest, "col", [(i, i ^ step) for i in range(16)]))
    units = jnp.square(jnp.concatenate(peaks, axis=0)[:, 0])

    page_shape = jax.ShapeDtypeStruct((PAGES * BS + SCALES, 128), jnp.int16)
    terms, *pages = pl.pallas_call(
        owner_kernel,
        out_shape=[jax.ShapeDtypeStruct((4, 4 * BS + 8, 128), jnp.int16)] + [page_shape] * 4,
        in_specs=[smem, smem, smem, smem, vmem, vmem],
        out_specs=[vmem] * 5,
        scratch_shapes=[
            pltpu.VMEM((128, BS, 128), jnp.float32),
            pltpu.VMEM((128, 1536), jnp.bfloat16),
            pltpu.VMEM((1536, 128), jnp.bfloat16),
            pltpu.VMEM((4, SCALES, 128), jnp.float32),
            pltpu.VMEM((4, 256, 128), jnp.float32),
        ],
        compiler_params=pltpu.CompilerParams(vmem_limit_bytes=24 * MIB),
        name="owner",
    )(ids, page_table, pattern, units, arrived, all_orbitals)
    terms = exchange(terms, "gz")
    for step in range(1, 4):
        pages[step] = lax.ppermute(pages[step], "gz", [(i, (i + step) % 4) for i in range(4)])
    sums = pl.pallas_call(
        term_kernel,
        out_shape=jax.ShapeDtypeStruct((256, 128), jnp.float32),
        in_specs=[vmem],
        out_specs=vmem,
        compiler_params=pltpu.CompilerParams(vmem_limit_bytes=4 * MIB),
        name="sums",
    )(terms)
    applied = jnp.sum(exchange(sums.reshape(16, 16, 128), "col"), axis=0)
    share = pl.pallas_call(
        share_kernel,
        out_shape=jax.ShapeDtypeStruct((1024, 128), jnp.float32),
        in_specs=[vmem] * 4,
        out_specs=vmem,
        compiler_params=pltpu.CompilerParams(vmem_limit_bytes=8 * MIB),
        name="share",
    )(*pages)
    return (share, applied)


def solution(mesh):
    placed = (
        P("row", "col"),
        P("row", "col"),
        P(),
        P("row", "col", "gz", None, None),
        P("row", "col", "gz"),
        P(("col", "gz"), None),
    )
    return jax.shard_map(
        shards,
        mesh=mesh,
        in_specs=placed,
        out_specs=(P("row", ("col", "gz")), P(("row", "col", "gz"), None)),
        check_vma=False,
    )
```

```python
import jax
import jax.numpy as jnp
from jax import lax
from jax.experimental import pallas as pl
from jax.experimental.pallas import tpu as pltpu
from jax.sharding import PartitionSpec as P


pbe_kappa = 0.804
pbe_mu = 0.2195149727645171
exch_const = 0.75 * (3.0 / 3.141592653589793) ** (1.0 / 3.0)
grad_scale = 4.0 * (3.0 * 3.141592653589793**2) ** (2.0 / 3.0)
density_floor = 0.2
spacing = 0.125


PLANE = ("row", "col")
BS = 64
MIB = 1024 * 1024
PAGES = 16
SCALES = 16
LEVELS = 32760.0


def with_halo(cells, sides, width):
    for axis, dim in sides:
        count = lax.axis_size(axis)
        head = lax.slice_in_dim(cells, 0, width, axis=dim)
        tail = lax.slice_in_dim(cells, cells.shape[dim] - width, cells.shape[dim], axis=dim)
        cells = jnp.concatenate(
            [
                lax.ppermute(tail, axis, [(i, (i + 1) % count) for i in range(count)]),
                cells,
                lax.ppermute(head, axis, [((i + 1) % count, i) for i in range(count)]),
            ],
            axis=dim,
        )
    return cells


def energy(density, grad_square):
    scaled = grad_square / (grad_scale * density ** (8.0 / 3.0))
    enhance = 1.0 + pbe_kappa - pbe_kappa / (1.0 + pbe_mu * scaled / pbe_kappa)
    return -exch_const * density ** (4.0 / 3.0) * enhance


def total_energy(density, grad_square):
    return jnp.sum(energy(density, grad_square))


def centered(grid_values, direction):
    higher = [slice(1, -1), slice(1, -1), slice(1, -1)]
    lesser = [slice(1, -1), slice(1, -1), slice(1, -1)]
    higher[direction] = slice(2, None)
    lesser[direction] = slice(None, -2)
    return (grid_values[tuple(higher)] - grid_values[tuple(lesser)]) / (2.0 * spacing)


def potential_deep(slab):
    padded = with_halo(slab, (("col", 1),), 2)
    gradients = [centered(padded, direction) for direction in range(3)]
    grad_square = (
        gradients[0] * gradients[0] + gradients[1] * gradients[1] + gradients[2] * gradients[2]
    )
    inner = padded[1:-1, 1:-1, 1:-1]
    first, second = jax.grad(total_energy, argnums=(0, 1))(inner, grad_square)
    divergence = centered(2.0 * second * gradients[0], 0)
    divergence = divergence + centered(2.0 * second * gradients[1], 1)
    divergence = divergence + centered(2.0 * second * gradients[2], 2)
    return first[1:-1, 1:-1, 1:-1] - divergence


def listed_pair(place, lists_ref, t):
    row, col, depth = place
    tile = t * 4 + depth
    a0 = lists_ref[2 * row, tile] - 16 * row
    a1 = lists_ref[2 * row + 1, tile] - 16 * row
    b = lists_ref[col, tile] - 8 * col
    return a0, a1, b


def lane_pair(low, high, rows):
    lane = lax.broadcasted_iota(jnp.int32, (rows, 128), 1)
    return jnp.where(lane < BS, low, high)


def pack_kernel(
    lists_ref, pattern_ref, matrix_hbm, out_hbm, pages_ref, matrix_ref, out_ref, held, in_sems, out_sems
):
    place = lax.axis_index("row"), lax.axis_index("col"), lax.axis_index("gz")

    def rows_in(q):
        rows = pl.ds(pl.multiple_of(q * 128, 128), 128)
        return pltpu.make_async_copy(matrix_hbm.at[rows], matrix_ref.at[rows], in_sems.at[q])

    def chunks_out(n):
        chunks = pl.ds(n * 16, 16)
        return pltpu.make_async_copy(out_ref.at[chunks], out_hbm.at[chunks], out_sems.at[n])

    for q in range(8):
        rows_in(q).start()

    def turn(q, carry):
        rows_in(q).wait()
        rows = pl.ds(pl.multiple_of(q * 128, 128), 128)
        first = (q < 4).astype(jnp.float32)
        for m in range(4):
            block = matrix_ref[rows, 128 * m : 128 * m + 128].T
            for half in range(2):
                b = 2 * m + half
                low = pattern_ref[b, 2 * q].astype(jnp.float32)
                high = pattern_ref[b, 2 * q + 1].astype(jnp.float32)
                part = block[BS * half : BS * half + BS]
                straight = lane_pair(low * first, high * (1.0 - first), BS).astype(jnp.bfloat16)
                crossed = lane_pair(low * (1.0 - first), high * first, BS).astype(jnp.bfloat16)
                held[b * 8 + q] = part * straight
                held[64 + b * 8 + q] = pltpu.roll(part * crossed, BS, 1)
        return carry

    lax.fori_loop(0, 8, turn, 0)

    def fill(t, carry):
        a0, a1, b = listed_pair(place, lists_ref, t)
        page0 = (a0 & 1) * 64 + b * 8 + (a0 >> 1)
        page1 = (1 - (a1 & 1)) * 64 + b * 8 + (a1 >> 1)
        pages_ref[t] = page0
        pages_ref[128 + t] = page1
        out_ref[t] = held[page0] + held[page1]
        return carry

    for n in range(8):
        lax.fori_loop(16 * n, 16 * n + 16, fill, 0, unroll=4)
        chunks_out(n).start()
    for n in range(8):
        chunks_out(n).wait()


def density_kernel(blocks_ref, phi_ref, core_ref, unit_ref, orbitals_ref, out_ref):
    def part(n, total):
        rows = pl.ds(pl.multiple_of(n * 256, 256), 256)
        left = jnp.concatenate([blocks_ref[r, rows, :] for r in range(8)], axis=1)
        product = jnp.dot(left, phi_ref[...], preferred_element_type=jnp.float32)
        return total + jnp.sum(phi_ref[rows, :].astype(jnp.float32) * product, axis=0, keepdims=True)

    rho = lax.fori_loop(0, 4, part, jnp.zeros((1, 384), jnp.float32))
    density = jnp.maximum(rho + core_ref[...], density_floor)
    out_ref[...] = jnp.broadcast_to(density[None], (32, 1, 384))


def slab_kernel(ids_ref, tiles_ref, out_ref):
    row, depth = ids_ref[0], ids_ref[2]
    line = lax.broadcasted_iota(jnp.int32, (16, 384), 0) * 24
    lane = lax.broadcasted_iota(jnp.int32, (16, 384), 1)
    own_line = (lane >= line) & (lane < line + 24)
    rows = []
    for across in (7, 0, 1):
        pieces = []
        for along in (3, 0, 1):
            place = lax.rem(row + across, 8) * 4 + lax.rem(depth + along, 4)
            pieces.append(jnp.where(own_line, jnp.broadcast_to(tiles_ref[place], (16, 384)), 0.0))
        rows.append(jnp.concatenate(pieces, axis=1))
    left = jnp.concatenate(rows, axis=0)
    source = lax.rem(lax.broadcasted_iota(jnp.int32, (1152, 128), 0), 24)
    piece = lax.broadcasted_iota(jnp.int32, (1152, 128), 0) // 384
    target = lax.broadcasted_iota(jnp.int32, (1152, 128), 1)
    wanted = source + 2 + 24 * (piece - 1)
    chosen = jnp.where((wanted == target) & (target < 28), 1.0, 0.0)
    slab = jnp.dot(left, chosen, precision=lax.Precision.HIGHEST, preferred_element_type=jnp.float32)
    out_ref[...] = slab.reshape(6, 8, 128)


def ham_kernel(scale_ref, phi_ref, field_ref, out_ref):
    def part(r, carry):
        rows = phi_ref[pl.ds(pl.multiple_of(r * 256, 256), 256), :].astype(jnp.float32)
        weighted = (rows * field_ref[...]).astype(jnp.bfloat16)
        block = lax.dot_general(
            phi_ref[...], weighted, (((1,), (1,)), ((), ())), preferred_element_type=jnp.float32
        )
        out_ref[2 * r] = block[:, 0:128] * scale_ref[0]
        out_ref[2 * r + 1] = block[:, 128:256] * scale_ref[0]
        return carry

    lax.fori_loop(0, 4, part, 0)


def coded(page):
    largest = jnp.max(jnp.abs(page), axis=0, keepdims=True)
    power = jnp.floor(jnp.log2(jnp.clip(largest, 1e-27, 1e27))) + 1.0
    levels = jnp.round(page * (jnp.exp2(-power) * LEVELS))
    return levels.astype(jnp.int32).astype(jnp.int16), power


def step_of(power):
    return jnp.exp2(power.astype(jnp.float32)) * (1.0 / LEVELS)


def owner_kernel(
    ids_ref,
    pages_ref,
    pattern_ref,
    scale_ref,
    blocks_ref,
    orbitals_ref,
    terms_ref,
    out0_ref,
    out1_ref,
    out2_ref,
    out3_ref,
    sums,
    factors,
    turned,
    powers,
    products,
):
    sums[...] = jnp.zeros_like(sums)

    def add(t, carry):
        page0, page1 = pages_ref[t], pages_ref[128 + t]
        block = blocks_ref[t] * scale_ref[8 * (((t & 15) ^ ids_ref[1]) >> 2)]
        sums[page0] += block
        sums[page1] += block
        return carry

    lax.fori_loop(0, 128, add, 0, unroll=4)
    outs = (out0_ref, out1_ref, out2_ref, out3_ref)

    orbitals = orbitals_ref[...]
    orbitals_high = orbitals.astype(jnp.bfloat16)
    orbitals_low = (orbitals - orbitals_high.astype(jnp.float32)).astype(jnp.bfloat16)
    factors[...] = jnp.concatenate([orbitals_high, orbitals_high, orbitals_low], axis=1)

    def finish(q, carry):
        first = (q < 4).astype(jnp.float32)
        for n, out in enumerate(outs):
            peer = lax.rem(ids_ref[2] + n, 4)
            for half in range(2):
                b = 2 * peer + half
                low = pattern_ref[b, 2 * q].astype(jnp.float32)
                high = pattern_ref[b, 2 * q + 1].astype(jnp.float32)
                straight = lane_pair(low * first, high * (1.0 - first), BS)
                crossed = lane_pair(high * first, low * (1.0 - first), BS)
                page = sums[b * 8 + q] * straight + pltpu.roll(sums[64 + b * 8 + q] * crossed, BS, 1)
                page_high = page.astype(jnp.bfloat16)
                page_low = (page - page_high.astype(jnp.float32)).astype(jnp.bfloat16)
                place = 2 * n + half
                turned[BS * place : BS * place + BS, :] = page_high
                turned[512 + BS * place : 512 + BS * place + BS, :] = page_low
                turned[1024 + BS * place : 1024 + BS * place + BS, :] = page_high
                levels, power = coded(page)
                place = half * 8 + q
                out[pl.ds(pl.multiple_of(place * BS, BS), BS), :] = levels
                powers[n, pl.ds(place, 1), :] = power
        part = jnp.dot(factors[...], turned[...], preferred_element_type=jnp.float32).T
        for half in range(2):
            for g in range(4):
                start = BS * half + 16 * g
                rows = pl.ds(pl.multiple_of((2 * q + half) * 16, 16), 16)
                products[g, rows, :] = part[start : start + 16]
        return carry

    lax.fori_loop(0, 8, finish, 0)
    for g in range(4):
        product_powers = []
        for n in range(4):
            levels, power = coded(products[g, BS * n : BS * n + BS, :])
            terms_ref[g, BS * n : BS * n + BS, :] = levels
            product_powers.append(power)
        terms_ref[g, 4 * BS : 4 * BS + 8, :] = (
            jnp.concatenate(product_powers * 2, axis=0).astype(jnp.int32).astype(jnp.int16)
        )
    for n, out in enumerate(outs):
        out[PAGES * BS : PAGES * BS + SCALES, :] = powers[n].astype(jnp.int32).astype(jnp.int16)


def term_kernel(coded_ref, out_ref):
    steps = [
        step_of(coded_ref[g, 4 * BS : 4 * BS + 8, :]) for g in range(4)
    ]
    for n in range(4):
        total = jnp.zeros((BS, 128), jnp.float32)
        for g in range(4):
            levels = coded_ref[g, BS * n : BS * n + BS, :].astype(jnp.float32)
            total = total + levels * steps[g][n : n + 1]
        out_ref[BS * n : BS * n + BS, :] = total


def share_kernel(coded0_ref, coded1_ref, coded2_ref, coded3_ref, out_ref):
    parts = (coded0_ref, coded1_ref, coded2_ref, coded3_ref)
    steps = [step_of(part[PAGES * BS : PAGES * BS + SCALES, :]) for part in parts]
    for q in range(8):
        halves = []
        for half in range(2):
            place = half * 8 + q
            total = jnp.zeros((BS, 128), jnp.float32)
            for part, step in zip(parts, steps):
                levels = part[place * BS : place * BS + BS, :].astype(jnp.float32)
                total = total + levels * step[place : place + 1]
            halves.append(total)
        out_ref[128 * q : 128 * q + 128, :] = jnp.concatenate(halves, axis=0).T


smem = pl.BlockSpec(memory_space=pltpu.SMEM)
vmem = pl.BlockSpec(memory_space=pltpu.VMEM)
anywhere = pl.BlockSpec(memory_space=pl.ANY)


def exchange(array, axes):
    return lax.all_to_all(array, axes, 0, 0, tiled=True)


def shards(density_matrix, block_pattern, tile_lists, basis_values, core_density, orbitals):
    ids = jnp.stack([lax.axis_index("row"), lax.axis_index("col"), lax.axis_index("gz")]).astype(jnp.int32)
    lists = tile_lists.T
    pattern = block_pattern.T
    phi = basis_values.reshape(1024, 384)

    outgoing, page_table = pl.pallas_call(
        pack_kernel,
        out_shape=[
            jax.ShapeDtypeStruct((128, BS, 128), jnp.bfloat16),
            jax.ShapeDtypeStruct((256,), jnp.int32),
        ],
        in_specs=[smem, smem, anywhere],
        out_specs=[anywhere, smem],
        scratch_shapes=[
            pltpu.VMEM((1024, 512), jnp.bfloat16),
            pltpu.VMEM((128, BS, 128), jnp.bfloat16),
            pltpu.VMEM((128, BS, 128), jnp.bfloat16),
            pltpu.SemaphoreType.DMA((8,)),
            pltpu.SemaphoreType.DMA((8,)),
        ],
        name="pack",
    )(lists, pattern, density_matrix)
    incoming = exchange(outgoing, PLANE)

    largest = jnp.full((8, 128), jnp.max(jnp.abs(phi)).astype(jnp.float32))
    for step in (1, 2, 4):
        other = lax.ppermute(largest, "row", [(i, i ^ step) for i in range(8)])
        largest = jnp.maximum(largest, other)
    others = []
    for step in (1, 2, 3):
        others.append(lax.ppermute(largest, "col", [(i, i ^ step) for i in range(16)]))
    for other in others:
        largest = jnp.maximum(largest, other)
    columns = [orbitals]
    for step in range(1, 4):
        columns.append(lax.ppermute(orbitals, "gz", [(i, (i - step) % 4) for i in range(4)]))
    all_orbitals = jnp.concatenate(columns, axis=0).T
    largest = jnp.maximum(largest, 1e-15)
    unit = jnp.square(largest)[0, 0:1]

    densities = pl.pallas_call(
        density_kernel,
        out_shape=jax.ShapeDtypeStruct((32, 1, 384), jnp.float32),
        in_specs=[vmem, vmem, vmem, anywhere, anywhere],
        out_specs=vmem,
        compiler_params=pltpu.CompilerParams(vmem_limit_bytes=12 * MIB),
        name="density",
    )(incoming.reshape(8, 1024, 128), phi, core_density.reshape(1, 384), unit, all_orbitals)
    slab = pl.pallas_call(
        slab_kernel,
        out_shape=jax.ShapeDtypeStruct((6, 8, 128), jnp.float32),
        in_specs=[smem, vmem],
        out_specs=vmem,
        compiler_params=pltpu.CompilerParams(vmem_limit_bytes=8 * MIB),
        name="slab",
    )(ids, exchange(densities, ("row", "gz")))
    field = potential_deep(slab[:, :, :28])

    local_ham = pl.pallas_call(
        ham_kernel,
        out_shape=jax.ShapeDtypeStruct((8, 1024, 128), jnp.float32),
        in_specs=[smem, vmem, vmem],
        out_specs=vmem,
        compiler_params=pltpu.CompilerParams(vmem_limit_bytes=16 * MIB),
        name="ham",
    )(1.0 / unit, phi, field.reshape(1, -1))
    returning = local_ham.astype(jnp.float16).reshape(128, BS, 128)
    arrived = exchange(returning, PLANE).astype(jnp.float32)
    peaks = [largest]
    for step in (4, 8, 12):
        peaks.append(lax.ppermute(largest, "col", [(i, i ^ step) for i in range(16)]))
    units = jnp.square(jnp.concatenate(peaks, axis=0)[:, 0])

    page_shape = jax.ShapeDtypeStruct((PAGES * BS + SCALES, 128), jnp.int16)
    terms, *pages = pl.pallas_call(
        owner_kernel,
        out_shape=[jax.ShapeDtypeStruct((4, 4 * BS + 8, 128), jnp.int16)] + [page_shape] * 4,
        in_specs=[smem, smem, smem, smem, vmem, vmem],
        out_specs=[vmem] * 5,
        scratch_shapes=[
            pltpu.VMEM((128, BS, 128), jnp.float32),
            pltpu.VMEM((128, 1536), jnp.bfloat16),
            pltpu.VMEM((1536, 128), jnp.bfloat16),
            pltpu.VMEM((4, SCALES, 128), jnp.float32),
            pltpu.VMEM((4, 256, 128), jnp.float32),
        ],
        compiler_params=pltpu.CompilerParams(vmem_limit_bytes=24 * MIB),
        name="owner",
    )(ids, page_table, pattern, units, arrived, all_orbitals)
    terms = exchange(terms, "gz")
    for step in range(1, 4):
        pages[step] = lax.ppermute(pages[step], "gz", [(i, (i + step) % 4) for i in range(4)])
    sums = pl.pallas_call(
        term_kernel,
        out_shape=jax.ShapeDtypeStruct((256, 128), jnp.float32),
        in_specs=[vmem],
        out_specs=vmem,
        compiler_params=pltpu.CompilerParams(vmem_limit_bytes=4 * MIB),
        name="sums",
    )(terms)
    applied = jnp.sum(exchange(sums.reshape(16, 16, 128), "col"), axis=0)
    share = pl.pallas_call(
        share_kernel,
        out_shape=jax.ShapeDtypeStruct((1024, 128), jnp.float32),
        in_specs=[vmem] * 4,
        out_specs=vmem,
        compiler_params=pltpu.CompilerParams(vmem_limit_bytes=8 * MIB),
        name="share",
    )(*pages)
    return (share, applied)


def solution(mesh):
    placed = (
        P("row", "col"),
        P("row", "col"),
        P(),
        P("row", "col", "gz", None, None),
        P("row", "col", "gz"),
        P(("col", "gz"), None),
    )
    return jax.shard_map(
        shards,
        mesh=mesh,
        in_specs=placed,
        out_specs=(P("row", ("col", "gz")), P(("row", "col", "gz"), None)),
        check_vma=False,
    )
```

```python
import jax
import jax.numpy as jnp
from jax import lax
from jax.experimental import pallas as pl
from jax.experimental.pallas import tpu as pltpu
from jax.sharding import PartitionSpec as P


pbe_kappa = 0.804
pbe_mu = 0.2195149727645171
exch_const = 0.75 * (3.0 / 3.141592653589793) ** (1.0 / 3.0)
grad_scale = 4.0 * (3.0 * 3.141592653589793**2) ** (2.0 / 3.0)
density_floor = 0.2
spacing = 0.125


PLANE = ("row", "col")
BS = 64
MIB = 1024 * 1024
PAGES = 16
SCALES = 16
LEVELS = 32760.0


def energy(density, grad_square):
    scaled = grad_square / (grad_scale * density ** (8.0 / 3.0))
    enhance = 1.0 + pbe_kappa - pbe_kappa / (1.0 + pbe_mu * scaled / pbe_kappa)
    return -exch_const * density ** (4.0 / 3.0) * enhance


def total_energy(density, grad_square):
    return jnp.sum(energy(density, grad_square))


def centered(grid_values, direction):
    higher = [slice(1, -1), slice(1, -1), slice(1, -1)]
    lesser = [slice(1, -1), slice(1, -1), slice(1, -1)]
    higher[direction] = slice(2, None)
    lesser[direction] = slice(None, -2)
    return (grid_values[tuple(higher)] - grid_values[tuple(lesser)]) / (2.0 * spacing)


def potential_deep(padded):
    gradients = [centered(padded, direction) for direction in range(3)]
    grad_square = (
        gradients[0] * gradients[0] + gradients[1] * gradients[1] + gradients[2] * gradients[2]
    )
    inner = padded[1:-1, 1:-1, 1:-1]
    first, second = jax.grad(total_energy, argnums=(0, 1))(inner, grad_square)
    divergence = centered(2.0 * second * gradients[0], 0)
    divergence = divergence + centered(2.0 * second * gradients[1], 1)
    divergence = divergence + centered(2.0 * second * gradients[2], 2)
    return first[1:-1, 1:-1, 1:-1] - divergence


def listed_pair(place, lists_ref, t):
    row, col, depth = place
    tile = t * 4 + depth
    a0 = lists_ref[2 * row, tile] - 16 * row
    a1 = lists_ref[2 * row + 1, tile] - 16 * row
    b = lists_ref[col, tile] - 8 * col
    return a0, a1, b


def lane_pair(low, high, rows):
    lane = lax.broadcasted_iota(jnp.int32, (rows, 128), 1)
    return jnp.where(lane < BS, low, high)


def pack_kernel(lists_ref, pattern_ref, matrix_ref, out_ref, pages_ref, held):
    place = lax.axis_index("row"), lax.axis_index("col"), lax.axis_index("gz")

    def turn(q, carry):
        rows = pl.ds(pl.multiple_of(q * 128, 128), 128)
        first = (q < 4).astype(jnp.float32)
        for m in range(4):
            block = matrix_ref[rows, 128 * m : 128 * m + 128].T
            for half in range(2):
                b = 2 * m + half
                low = pattern_ref[b, 2 * q].astype(jnp.float32)
                high = pattern_ref[b, 2 * q + 1].astype(jnp.float32)
                part = block[BS * half : BS * half + BS]
                straight = lane_pair(low * first, high * (1.0 - first), BS).astype(jnp.bfloat16)
                crossed = lane_pair(low * (1.0 - first), high * first, BS).astype(jnp.bfloat16)
                held[b * 8 + q] = part * straight
                held[64 + b * 8 + q] = pltpu.roll(part * crossed, BS, 1)
        return carry

    lax.fori_loop(0, 8, turn, 0)

    def fill(t, carry):
        a0, a1, b = listed_pair(place, lists_ref, t)
        page0 = (a0 & 1) * 64 + b * 8 + (a0 >> 1)
        page1 = (1 - (a1 & 1)) * 64 + b * 8 + (a1 >> 1)
        pages_ref[t] = page0
        pages_ref[128 + t] = page1
        out_ref[t] = held[page0] + held[page1]
        return carry

    lax.fori_loop(0, 128, fill, 0, unroll=4)


def density_kernel(blocks_ref, phi_ref, core_ref, unit_ref, orbitals_ref, out_ref):
    def part(n, total):
        rows = pl.ds(pl.multiple_of(n * 256, 256), 256)
        left = jnp.concatenate([blocks_ref[r, rows, :] for r in range(8)], axis=1)
        product = jnp.dot(left, phi_ref[...], preferred_element_type=jnp.float32)
        return total + jnp.sum(phi_ref[rows, :].astype(jnp.float32) * product, axis=0, keepdims=True)

    rho = lax.fori_loop(0, 4, part, jnp.zeros((1, 384), jnp.float32))
    density = jnp.maximum(rho + core_ref[...], density_floor)
    out_ref[...] = jnp.broadcast_to(density[None], (32, 1, 384))


def slab_kernel(tiles_ref, out_ref, head_ref, tail_ref):
    row, depth = lax.axis_index("row"), lax.axis_index("gz")
    line = lax.broadcasted_iota(jnp.int32, (16, 384), 0) * 24
    lane = lax.broadcasted_iota(jnp.int32, (16, 384), 1)
    own_line = (lane >= line) & (lane < line + 24)
    rows = []
    for across in (7, 0, 1):
        pieces = []
        for along in (3, 0, 1):
            place = lax.rem(row + across, 8) * 4 + lax.rem(depth + along, 4)
            pieces.append(jnp.where(own_line, jnp.broadcast_to(tiles_ref[place], (16, 384)), 0.0))
        rows.append(jnp.concatenate(pieces, axis=1))
    left = jnp.concatenate(rows, axis=0)
    source = lax.rem(lax.broadcasted_iota(jnp.int32, (1152, 128), 0), 24)
    piece = lax.broadcasted_iota(jnp.int32, (1152, 128), 0) // 384
    target = lax.broadcasted_iota(jnp.int32, (1152, 128), 1)
    wanted = source + 2 + 24 * (piece - 1)
    chosen = jnp.where((wanted == target) & (target < 28), 1.0, 0.0)
    slab = jnp.dot(left, chosen, precision=lax.Precision.HIGHEST, preferred_element_type=jnp.float32)
    slab = slab.reshape(6, 8, 128)
    out_ref[...] = slab
    head_ref[...] = slab[:, 0:2]
    tail_ref[...] = slab[:, 6:8]


def ham_kernel(scale_ref, phi_ref, field_ref, out_ref):
    def part(r, carry):
        rows = phi_ref[pl.ds(pl.multiple_of(r * 256, 256), 256), :].astype(jnp.float32)
        weighted = (rows * field_ref[...]).astype(jnp.bfloat16)
        block = lax.dot_general(
            phi_ref[...], weighted, (((1,), (1,)), ((), ())), preferred_element_type=jnp.float32
        )
        out_ref[2 * r] = block[:, 0:128] * scale_ref[0]
        out_ref[2 * r + 1] = block[:, 128:256] * scale_ref[0]
        return carry

    lax.fori_loop(0, 4, part, 0)


def coded(page):
    largest = jnp.max(jnp.abs(page), axis=0, keepdims=True)
    power = jnp.floor(jnp.log2(jnp.clip(largest, 1e-27, 1e27))) + 1.0
    levels = jnp.round(page * (jnp.exp2(-power) * LEVELS))
    return levels.astype(jnp.int32).astype(jnp.int16), power


def step_of(power):
    return jnp.exp2(power.astype(jnp.float32)) * (1.0 / LEVELS)


def owner_kernel(
    pages_ref,
    pattern_ref,
    scale_ref,
    blocks_ref,
    orbitals_ref,
    terms_ref,
    out0_ref,
    out1_ref,
    out2_ref,
    out3_ref,
    sums,
    factors,
    turned,
    powers,
    products,
):
    col, depth = lax.axis_index("col"), lax.axis_index("gz")
    sums[...] = jnp.zeros_like(sums)

    def add(t, carry):
        page0, page1 = pages_ref[t], pages_ref[128 + t]
        block = blocks_ref[t] * scale_ref[8 * (((t & 15) ^ col) >> 2)]
        sums[page0] += block
        sums[page1] += block
        return carry

    lax.fori_loop(0, 128, add, 0, unroll=4)
    outs = (out0_ref, out1_ref, out2_ref, out3_ref)

    orbitals = orbitals_ref[...]
    orbitals_high = orbitals.astype(jnp.bfloat16)
    orbitals_low = (orbitals - orbitals_high.astype(jnp.float32)).astype(jnp.bfloat16)
    factors[...] = jnp.concatenate([orbitals_high, orbitals_high, orbitals_low], axis=1)

    def finish(q, carry):
        first = (q < 4).astype(jnp.float32)
        for n, out in enumerate(outs):
            peer = lax.rem(depth + n, 4)
            for half in range(2):
                b = 2 * peer + half
                low = pattern_ref[b, 2 * q].astype(jnp.float32)
                high = pattern_ref[b, 2 * q + 1].astype(jnp.float32)
                straight = lane_pair(low * first, high * (1.0 - first), BS)
                crossed = lane_pair(high * first, low * (1.0 - first), BS)
                page = sums[b * 8 + q] * straight + pltpu.roll(sums[64 + b * 8 + q] * crossed, BS, 1)
                page_high = page.astype(jnp.bfloat16)
                page_low = (page - page_high.astype(jnp.float32)).astype(jnp.bfloat16)
                place = 2 * n + half
                turned[BS * place : BS * place + BS, :] = page_high
                turned[512 + BS * place : 512 + BS * place + BS, :] = page_low
                turned[1024 + BS * place : 1024 + BS * place + BS, :] = page_high
                levels, power = coded(page)
                place = half * 8 + q
                out[pl.ds(pl.multiple_of(place * BS, BS), BS), :] = levels
                powers[n, pl.ds(place, 1), :] = power
        part = jnp.dot(factors[...], turned[...], preferred_element_type=jnp.float32).T
        for half in range(2):
            for g in range(4):
                start = BS * half + 16 * g
                rows = pl.ds(pl.multiple_of((2 * q + half) * 16, 16), 16)
                products[g, rows, :] = part[start : start + 16]
        return carry

    lax.fori_loop(0, 8, finish, 0)
    for g in range(4):
        product_powers = []
        for n in range(4):
            levels, power = coded(products[g, BS * n : BS * n + BS, :])
            terms_ref[g, BS * n : BS * n + BS, :] = levels
            product_powers.append(power)
        terms_ref[g, 4 * BS : 4 * BS + 8, :] = (
            jnp.concatenate(product_powers * 2, axis=0).astype(jnp.int32).astype(jnp.int16)
        )
    for n, out in enumerate(outs):
        out[PAGES * BS : PAGES * BS + SCALES, :] = powers[n].astype(jnp.int32).astype(jnp.int16)


def term_kernel(coded_ref, out_ref):
    steps = [
        step_of(coded_ref[g, 4 * BS : 4 * BS + 8, :]) for g in range(4)
    ]
    for n in range(4):
        total = jnp.zeros((BS, 128), jnp.float32)
        for g in range(4):
            levels = coded_ref[g, BS * n : BS * n + BS, :].astype(jnp.float32)
            total = total + levels * steps[g][n : n + 1]
        out_ref[BS * n : BS * n + BS, :] = total


def share_kernel(coded0_ref, coded1_ref, coded2_ref, coded3_ref, out_ref):
    parts = (coded0_ref, coded1_ref, coded2_ref, coded3_ref)
    steps = [step_of(part[PAGES * BS : PAGES * BS + SCALES, :]) for part in parts]
    for q in range(8):
        halves = []
        for half in range(2):
            place = half * 8 + q
            total = jnp.zeros((BS, 128), jnp.float32)
            for part, step in zip(parts, steps):
                levels = part[place * BS : place * BS + BS, :].astype(jnp.float32)
                total = total + levels * step[place : place + 1]
            halves.append(total)
        out_ref[128 * q : 128 * q + 128, :] = jnp.concatenate(halves, axis=0).T


smem = pl.BlockSpec(memory_space=pltpu.SMEM)
vmem = pl.BlockSpec(memory_space=pltpu.VMEM)
anywhere = pl.BlockSpec(memory_space=pl.ANY)


def exchange(array, axes):
    return lax.all_to_all(array, axes, 0, 0, tiled=True)


def shards(density_matrix, block_pattern, tile_lists, basis_values, core_density, orbitals):
    lists = tile_lists.T
    pattern = block_pattern.T
    phi = basis_values.reshape(1024, 384)

    outgoing, page_table = pl.pallas_call(
        pack_kernel,
        out_shape=[
            jax.ShapeDtypeStruct((128, BS, 128), jnp.bfloat16),
            jax.ShapeDtypeStruct((256,), jnp.int32),
        ],
        in_specs=[smem, smem, vmem],
        out_specs=[vmem, smem],
        scratch_shapes=[pltpu.VMEM((128, BS, 128), jnp.bfloat16)],
        name="pack",
    )(lists, pattern, density_matrix)
    incoming = exchange(outgoing, PLANE)

    largest = jnp.full((8, 128), jnp.max(jnp.abs(phi)).astype(jnp.float32))
    for step in (1, 2, 4):
        other = lax.ppermute(largest, "row", [(i, i ^ step) for i in range(8)])
        largest = jnp.maximum(largest, other)
    others = []
    for step in (1, 2, 3):
        others.append(lax.ppermute(largest, "col", [(i, i ^ step) for i in range(16)]))
    for other in others:
        largest = jnp.maximum(largest, other)
    columns = [orbitals]
    for step in range(1, 4):
        columns.append(lax.ppermute(orbitals, "gz", [(i, (i - step) % 4) for i in range(4)]))
    all_orbitals = jnp.concatenate(columns, axis=0).T
    largest = jnp.maximum(largest, 1e-15)
    unit = jnp.square(largest)[0, 0:1]

    densities = pl.pallas_call(
        density_kernel,
        out_shape=jax.ShapeDtypeStruct((32, 1, 384), jnp.float32),
        in_specs=[vmem, vmem, vmem, anywhere, anywhere],
        out_specs=vmem,
        compiler_params=pltpu.CompilerParams(vmem_limit_bytes=12 * MIB),
        name="density",
    )(incoming.reshape(8, 1024, 128), phi, core_density.reshape(1, 384), unit, all_orbitals)
    edge = jax.ShapeDtypeStruct((6, 2, 128), jnp.float32)
    slab, head, tail = pl.pallas_call(
        slab_kernel,
        out_shape=[jax.ShapeDtypeStruct((6, 8, 128), jnp.float32), edge, edge],
        in_specs=[vmem],
        out_specs=[vmem] * 3,
        compiler_params=pltpu.CompilerParams(vmem_limit_bytes=8 * MIB),
        name="slab",
    )(exchange(densities, ("row", "gz")))
    lower = lax.ppermute(tail, "col", [(i, (i + 1) % 16) for i in range(16)])
    upper = lax.ppermute(head, "col", [((i + 1) % 16, i) for i in range(16)])
    field = potential_deep(jnp.concatenate([lower, slab, upper], axis=1)[:, :, :28])

    local_ham = pl.pallas_call(
        ham_kernel,
        out_shape=jax.ShapeDtypeStruct((8, 1024, 128), jnp.float32),
        in_specs=[smem, vmem, vmem],
        out_specs=vmem,
        compiler_params=pltpu.CompilerParams(vmem_limit_bytes=16 * MIB),
        name="ham",
    )(1.0 / unit, phi, field.reshape(1, -1))
    returning = local_ham.astype(jnp.float16).reshape(128, BS, 128)
    arrived = exchange(returning, PLANE).astype(jnp.float32)
    peaks = [largest]
    for step in (4, 8, 12):
        peaks.append(lax.ppermute(largest, "col", [(i, i ^ step) for i in range(16)]))
    units = jnp.square(jnp.concatenate(peaks, axis=0)[:, 0])

    page_shape = jax.ShapeDtypeStruct((PAGES * BS + SCALES, 128), jnp.int16)
    terms, *pages = pl.pallas_call(
        owner_kernel,
        out_shape=[jax.ShapeDtypeStruct((4, 4 * BS + 8, 128), jnp.int16)] + [page_shape] * 4,
        in_specs=[smem, smem, smem, vmem, vmem],
        out_specs=[vmem] * 5,
        scratch_shapes=[
            pltpu.VMEM((128, BS, 128), jnp.float32),
            pltpu.VMEM((128, 1536), jnp.bfloat16),
            pltpu.VMEM((1536, 128), jnp.bfloat16),
            pltpu.VMEM((4, SCALES, 128), jnp.float32),
            pltpu.VMEM((4, 256, 128), jnp.float32),
        ],
        compiler_params=pltpu.CompilerParams(vmem_limit_bytes=24 * MIB),
        name="owner",
    )(page_table, pattern, units, arrived, all_orbitals)
    terms = exchange(terms, "gz")
    for step in range(1, 4):
        pages[step] = lax.ppermute(pages[step], "gz", [(i, (i + step) % 4) for i in range(4)])
    sums = pl.pallas_call(
        term_kernel,
        out_shape=jax.ShapeDtypeStruct((256, 128), jnp.float32),
        in_specs=[vmem],
        out_specs=vmem,
        compiler_params=pltpu.CompilerParams(vmem_limit_bytes=4 * MIB),
        name="sums",
    )(terms)
    applied = jnp.sum(exchange(sums.reshape(16, 16, 128), "col"), axis=0)
    share = pl.pallas_call(
        share_kernel,
        out_shape=jax.ShapeDtypeStruct((1024, 128), jnp.float32),
        in_specs=[vmem] * 4,
        out_specs=vmem,
        compiler_params=pltpu.CompilerParams(vmem_limit_bytes=8 * MIB),
        name="share",
    )(*pages)
    return (share, applied)


def solution(mesh):
    placed = (
        P("row", "col"),
        P("row", "col"),
        P(),
        P("row", "col", "gz", None, None),
        P("row", "col", "gz"),
        P(("col", "gz"), None),
    )
    return jax.shard_map(
        shards,
        mesh=mesh,
        in_specs=placed,
        out_specs=(P("row", ("col", "gz")), P(("row", "col", "gz"), None)),
        check_vma=False,
    )
```
